32 devices in a mesh: section: 2 (over x), view: 8 (over z, y), scene: 2 (over core).
Axes of the slice: x: 2, y: 2, z: 4, core: 2. Of those that a mesh axis runs over, the one named last changes fastest.
Arguments:
- tokens: bfloat16 [2, 512, 1024], P('scene', ('section', 'view')), may hold values from -6 to 6
- norm_gain: float32 [1024], replicated, may hold values from 0.1 to 1.9
- head_weight: bfloat16 [1024, 512], replicated, may hold values from -0.1875 to 0.1875
- tile_lists: int32 [2, 64, 128], P('scene', ('section', 'view')), may hold values from 0 to 32767, as said below
- tile_counts: int32 [2, 64], P('scene', ('section', 'view')), may hold values from 1 to 128, as said below
- cameras: float32 [2, 2, 8], P('scene'), may hold values from -3 to 3
- targets: bfloat16 [2, 64, 768], P('scene', ('section', 'view')), may hold values from 0 to 1
Outputs:
- image: bfloat16 [2, 64, 768], P('scene', ('section', 'view'))
- grad_head: float32 [1024, 512], replicated
- loss: float32 [], replicated
The draws below stay inside these ranges and needn't reach their ends.
Inputs may be any that keep to these rules, and one draw needn't show every extreme that they name: `tile_lists`: gaussian n of a scene has owner n // 2048. Among the 512 slots (live or not) of each aligned block of 4 tiles, at most 64 name Gaussians of one owner, and in every such block some owner is named exactly 64 times. `tile_counts`: the first tile of each scene has 128 live slots.
All inputs are finite; a program needn't handle non-finite values.
Results may differ from the reference program's by a relative error of at most 0.014.
Values may be sent and summed in bfloat16 or wider, within the bound.
A program may use at most 256 MiB of HBM per device.

```python
import jax
import jax.numpy as jnp
from jax import lax

D = 1024
GPT = 64
PARAMS = 8
K = 128
SIDE = 16
VIEWS = 2
TOK_DEV = 32
TILE_DEV = 4
SCENES = 2
TOKENS = 512
GAUSS = 32768
TILES = 64
OUTW = 512
CAP = 64


def draw_tile_counts(key, part):
    first, second = jax.random.split(jax.random.fold_in(key, 17))
    raw = jax.random.randint(first, (SCENES, TILES), 1, K + 1)
    heavy = jax.random.randint(second, (SCENES, TILES // TILE_DEV, 1), 0, 2)
    light = (raw + 3) // 4
    counts = jnp.where(heavy == 1, raw.reshape(SCENES, TILES // TILE_DEV, TILE_DEV), light.reshape(SCENES, TILES // TILE_DEV, TILE_DEV))
    counts = counts.reshape(SCENES, TILES)
    return counts.at[:, 0].set(K).astype(jnp.int32)


def draw_tile_lists(key, part):
    first, second, third = jax.random.split(jax.random.fold_in(key, 29), 3)
    owners = TILES // TILE_DEV
    slot_total = TILE_DEV * K
    blocks = SCENES * owners
    own_count = TOK_DEV * GPT
    busiest = jax.random.randint(first, (blocks, 1), 0, owners)
    place = jnp.arange(slot_total, dtype=jnp.int32)[None, :]
    others = (busiest + 1 + (place - CAP) % (owners - 1)) % owners
    owner = jnp.where(place < CAP, busiest, others)
    scores = jax.random.randint(second, (blocks, slot_total), 0, slot_total) * slot_total + place
    order = jnp.argsort(scores, axis=1)
    owner = jnp.take_along_axis(owner, order, axis=1)
    within = jax.random.randint(third, (blocks, slot_total), 0, own_count)
    lists = owner * own_count + within
    return lists.reshape(SCENES, TILES, K).astype(jnp.int32)


def shard_levels(stream_key, extent, cuts, smallest, top_value):
    def one(position, parts):
        draws = jax.random.uniform(jax.random.fold_in(jax.random.fold_in(stream_key, 6), position), (parts,), jnp.float32, smallest / len(cuts), top_value / len(cuts))
        return jnp.repeat(jnp.exp(draws), extent[position] // parts).reshape((-1,) + (1,) * (len(extent) - position - 1))

    factor_of = one(*cuts[0])
    for cut in cuts[1:]:
        factor_of = factor_of * one(*cut)
    return factor_of


def scatter_about(rng, extent, width, limit, pieces=(), held_as=jnp.bfloat16):
    values = width * jax.random.normal(rng, extent, jnp.float32)
    if pieces:
        values = values * shard_levels(rng, extent, pieces, -0.22, 0.18)
    return jnp.clip(values, -limit, limit).astype(held_as)


def setup_inputs(seed: int = 0) -> dict:
    seeds = jax.random.split(jax.random.key(seed), 8)
    return {
        "tokens": scatter_about(seeds[0], (SCENES, TOKENS, D), 1.0, 6.0, ((0, 2), (1, 16))),
        "norm_gain": jnp.clip(1.0 + 0.18 * jax.random.normal(seeds[1], (D,), jnp.float32), 0.1, 1.9),
        "head_weight": scatter_about(seeds[2], (D, OUTW), D ** -0.5, 0.1875),
        "tile_lists": draw_tile_lists(jax.random.fold_in(seeds[7], 71), 0),
        "tile_counts": draw_tile_counts(jax.random.fold_in(seeds[7], 71), 0),
        "cameras": scatter_about(seeds[5], (SCENES, VIEWS, 8), 0.8, 3.0, ((0, 2),), jnp.float32),
        "targets": jnp.clip(1.0 * jax.random.uniform(seeds[6], (SCENES, TILES, 3 * SIDE * SIDE), jnp.float32) ** shard_levels(seeds[6], (SCENES, TILES, 3 * SIDE * SIDE), ((0, 2), (1, 16)), -0.2, 0.2), 0.0, 1.0).astype(jnp.bfloat16),
    }


def pixel_grid():
    place = jnp.arange(SIDE * SIDE, dtype=jnp.int32)
    across = ((place % SIDE).astype(jnp.float32) + 0.5) * (2.0 / SIDE) - 1.0
    down = ((place // SIDE).astype(jnp.float32) + 0.5) * (2.0 / SIDE) - 1.0
    return (across, down)

def composite(values, live, cams, wanted, across, down):
    slots = jnp.arange(K, dtype=jnp.int32)
    strict = (slots[:, None] < slots[None, :]).astype(jnp.float32)
    sx = jnp.tanh(cams[:, 0:1] * values[0] + cams[:, 1:2] * values[1] + cams[:, 2:3] * values[2] + cams[:, 3:4])
    sy = jnp.tanh(cams[:, 4:5] * values[0] + cams[:, 5:6] * values[1] + cams[:, 6:7] * values[2] + cams[:, 7:8])
    spread = jnp.exp(-2.0 * values[3])
    dxx = across[None, None, :] - sx[:, :, None]
    dyy = down[None, None, :] - sy[:, :, None]
    alpha = 0.3 * jax.nn.sigmoid(values[4])[:, :, None] * jnp.exp(-0.5 * (dxx * dxx + dyy * dyy) * spread[:, :, None]) * live[:, :, None]
    logs = jnp.log1p(-alpha)
    before = jnp.einsum('bkp,kj->bjp', logs, strict, precision=lax.Precision.HIGHEST)
    weight = alpha * jnp.exp(before)
    colour = jnp.einsum('bkp,cbk->bcp', weight, jax.nn.sigmoid(values[5:8]), precision=lax.Precision.HIGHEST)
    colour = colour.reshape(colour.shape[0], 3 * SIDE * SIDE)
    diff = colour - wanted.astype(jnp.float32)
    return (jnp.sum(diff * diff), colour)

def normalize(tokens_scene, norm_gain):
    values = tokens_scene.astype(jnp.float32)
    scale = lax.rsqrt(lax.optimization_barrier(jnp.mean(values * values, axis=-1, keepdims=True)) + 1e-06)
    return (values * scale * norm_gain).astype(jnp.bfloat16)

def scene_pass(tokens_scene, norm_gain, head_weight, lists, counts, cams, wanted, factor):
    normed = normalize(tokens_scene, norm_gain)
    head = jnp.dot(normed, head_weight, preferred_element_type=jnp.float32)
    gauss = head.reshape(TOKENS, PARAMS, GPT).transpose(1, 0, 2).reshape(PARAMS, GAUSS).astype(jnp.bfloat16)
    gauss_f = gauss.astype(jnp.float32)
    per_view = TILES // VIEWS
    which = jnp.arange(TILES, dtype=jnp.int32) // per_view
    onehot = (which[:, None] == jnp.arange(VIEWS, dtype=jnp.int32)[None, :]).astype(jnp.float32)
    tile_cams = jnp.dot(onehot, cams, precision=lax.Precision.HIGHEST)
    blocks = TILES // TILE_DEV
    across, down = pixel_grid()
    slots = jnp.arange(K, dtype=jnp.int32)

    def step(carry, inputs):
        dense, total = carry
        lb, cb, camb, wb = inputs
        values = jnp.take(gauss_f, lb.astype(jnp.int32), axis=1)
        live = (slots[None, :] < cb[:, None]).astype(jnp.float32)

        def local(vals):
            return composite(vals, live, camb, wb, across, down)
        part, pullback, colour = jax.vjp(local, values, has_aux=True)
        grads = pullback(jnp.ones_like(part) * factor)[0]
        dense = dense.at[:, lb.reshape(-1)].add(grads.reshape(PARAMS, -1))
        return ((dense, total + part * factor), colour.astype(jnp.bfloat16))
    start = (jnp.zeros((PARAMS, GAUSS), jnp.float32), jnp.zeros((), jnp.float32))
    inputs = (lists.reshape(blocks, TILE_DEV, K), counts.reshape(blocks, TILE_DEV), tile_cams.reshape(blocks, TILE_DEV, 8), wanted.reshape(blocks, TILE_DEV, 3 * SIDE * SIDE))
    (dense, total), images = lax.scan(step, start, inputs)
    dhead = dense.reshape(PARAMS, TOKENS, GPT).transpose(1, 0, 2).reshape(TOKENS, PARAMS * GPT)
    grad = jnp.dot(normed.astype(jnp.float32).T, dhead, precision=lax.Precision.HIGHEST)
    return (images.reshape(TILES, 3 * SIDE * SIDE), grad, total)

def reference(tokens, norm_gain, head_weight, tile_lists, tile_counts, cameras, targets):
    factor = 1.0 / (SCENES * TILES)
    images = []
    grad_head = jnp.zeros((D, PARAMS * GPT), jnp.float32)
    loss = jnp.zeros((), jnp.float32)
    for scene in range(SCENES):
        image_s, grad_s, loss_s = scene_pass(tokens[scene], norm_gain, head_weight, tile_lists[scene], tile_counts[scene], cameras[scene], targets[scene], factor)
        images.append(image_s)
        grad_head = grad_head + grad_s
        loss = loss + loss_s
    return (jnp.stack(images), grad_head, loss)
```

```python
import functools

import jax
import jax.numpy as jnp
from jax import lax
from jax.experimental import pallas as pl
from jax.experimental.pallas import tpu as pltpu
from jax.sharding import PartitionSpec as P

PARAMS = 8
SIDE = 16
VIEWS = 2
MESH = pl.DeviceIdType.MESH
F32 = jnp.float32
BF16 = jnp.bfloat16
NN = (((1,), (0,)), ((), ()))
NT = (((1,), (1,)), ((), ()))
TN = (((0,), (0,)), ((), ()))


def mm(a, b, dims):
    return lax.dot_general(a, b, dims, preferred_element_type=F32)


def split(x):
    hi = x.astype(BF16)
    lo = (x - hi.astype(F32)).astype(BF16)
    return hi, lo


def mm2(a, x, dims):
    hi, lo = split(x)
    return mm(a, hi, dims) + mm(a, lo, dims)


def mm3(x, y, dims):
    xh, xl = split(x)
    yh, yl = split(y)
    return mm(xh, yh, dims) + mm(xh, yl, dims) + mm(xl, yh, dims)


def sigmoid(x):
    return 1.0 / (1.0 + jnp.exp(-x))


def turn(a, k, n):
    if n & (n - 1):
        return lax.rem(a + k, n)
    out, bit = 0, 1
    while bit < n:
        out = out + bit * lax.rem((a // bit) + (k // bit), 2)
        bit *= 2
    return out


def kernel(
    nsec, nview, factor,
    tok_hbm, gain_hbm, w_hbm, list_hbm, count_ref, cam_ref, want_hbm,
    image_ref, grad_ref, loss_ref,
    tok_ref, gain_ref, w_ref, list_ref, want_ref,
    perm, asked, wanted, found, given, lists, where, fits, norms, grads, dhead, mine, theirs,
    losses, loss_mine, loss_theirs,
    s_in, s_small, r_small, s_norm, r_norm, s_grad, r_grad, s_part, r_part, s_loss, r_loss,
):
    group = nsec * nview
    nlo = 2 if nview % 2 == 0 else 1
    nhi = nview // nlo
    sec, view, scene = lax.axis_index("section"), lax.axis_index("view"), lax.axis_index("scene")
    hi, lo = view // nlo, lax.rem(view, nlo)
    me = sec * nview + view
    tok_rows, width = tok_ref.shape
    outw = w_ref.shape[1]
    gpt = outw // PARAMS
    tiles, K = list_ref.shape
    slots = tiles * K
    tokens = group * tok_rows
    pix = SIDE * SIDE
    cap = 2 * slots // group
    per = 128 // cap
    packs = group // per
    ahead = where.shape[0] > 1

    def local(n, src, dst):
        return pltpu.make_async_copy(src, dst, s_in.at[n])

    loads = [
        local(0, list_hbm, list_ref),
        local(1, tok_hbm, tok_ref),
        local(2, gain_hbm, gain_ref),
        local(3, w_hbm, w_ref),
        local(4, want_hbm, want_ref),
    ]
    for load in loads:
        load.start()

    def peer(i):
        s = turn(sec, lax.rem(i, nsec), nsec)
        l = turn(lo, lax.rem(i // nsec, nlo), nlo)
        h = turn(hi, i // (nsec * nlo), nhi)
        v = h * nlo + l
        return s * nview + v, (s, v, scene)

    def place_of(s, l, h):
        return (s * nlo + l) * nhi + h

    partner = (sec, view, 1 - scene)
    barrier = pltpu.get_barrier_semaphore()

    @pl.loop(1, group)
    def _(i):
        pl.semaphore_signal(barrier, inc=1, device_id=peer(i)[1], device_id_type=MESH)

    pl.semaphore_signal(barrier, inc=1, device_id=partner, device_id_type=MESH)

    loads[0].wait()
    number = jnp.concatenate([list_ref[pl.ds(b, 1), :] for b in range(tiles)], axis=1)
    token = number // gpt
    gauss = number - token * gpt
    owner = token // tok_rows
    inner = token - owner * tok_rows
    ow_sec = owner // nview
    ow_hi = (owner - ow_sec * nview) // nlo
    ow_lo = owner - ow_sec * nview - ow_hi * nlo
    row = place_of(ow_sec, ow_lo, ow_hi) * tok_rows + inner
    for b in range(tiles):
        cut = slice(b * K, (b + 1) * K)
        lists[me, pl.ds(b, 1), :] = row[:, cut]
        lists[me, pl.ds(tiles + b, 1), :] = gauss[:, cut]
    mask = jnp.where(lax.broadcasted_iota(jnp.int32, (group, slots), 0) == owner, 1.0, 0.0)
    earlier = jnp.where(
        lax.broadcasted_iota(jnp.int32, (slots, slots), 0)
        < lax.broadcasted_iota(jnp.int32, (slots, slots), 1),
        1.0, 0.0,
    ).astype(BF16)
    rank = jnp.sum(mask * mm(mask.astype(BF16), earlier, NN), axis=0, keepdims=True)
    dest = owner * cap + rank.astype(jnp.int32)
    perm[...] = jnp.where(
        lax.broadcasted_iota(jnp.int32, (group * cap, slots), 0) == dest, 1.0, 0.0
    ).astype(BF16)
    asks = jnp.concatenate(
        [inner.astype(F32), gauss.astype(F32), jnp.zeros((6, slots), F32)], axis=0
    ).astype(BF16)
    requests = mm(asks, perm[...], NT)
    for i in range(packs):
        asked[i] = requests[:, i * 128 : (i + 1) * 128]
    wanted[me] = asked[me // per]

    pl.semaphore_wait(barrier, group)

    def small(n, src, dst, where_to):
        return pltpu.make_async_remote_copy(
            src_ref=src, dst_ref=dst, send_sem=s_small.at[n], recv_sem=r_small.at[n],
            device_id=where_to, device_id_type=MESH,
        )

    def all_small(n, buf):
        span = buf.at[pl.ds(0, group - 1)]
        return small(n, span, span, partner)

    @pl.loop(1, group)
    def _(i):
        j, to = peer(i)
        small(0, asked.at[j // per], wanted.at[me], to).start()

    @pl.loop(1, group)
    def _(i):
        small(1, lists.at[me], lists.at[me], peer(i)[1]).start()

    loads[1].wait()
    loads[2].wait()
    spot = place_of(sec, lo, hi)
    x = tok_ref[...].astype(F32)
    scale = lax.rsqrt(jnp.mean(x * x, axis=-1, keepdims=True) + 1e-06)
    normed = (x * scale * gain_ref[...]).astype(BF16)
    norms[spot] = normed

    def norm_copy(n, span, to):
        return pltpu.make_async_remote_copy(
            src_ref=norms.at[span], dst_ref=norms.at[span], send_sem=s_norm.at[n],
            recv_sem=r_norm.at[n], device_id=to, device_id_type=MESH,
        )

    def line_copy(k):
        h = turn(hi, k, nhi)
        return norm_copy(0, pl.ds(spot, 1), (sec, h * nlo + lo, scene))

    line = pl.ds((sec * nlo + lo) * nhi, nhi)
    beside = [(turn(sec, k, nsec), lo) for k in range(1, nsec)]
    below = [(sec, turn(lo, k, nlo)) for k in range(1, nlo)]

    @pl.loop(1, nhi)
    def _(k):
        line_copy(k).start()

    loads[3].wait()
    head = mm(normed, w_ref[...], NN)
    stack = jnp.concatenate(
        [head[:, p * gpt : (p + 1) * gpt] for p in range(PARAMS)], axis=0
    ).astype(BF16)
    er = lax.broadcasted_iota(jnp.int32, (PARAMS * tok_rows, PARAMS * tok_rows), 0)
    ec = lax.broadcasted_iota(jnp.int32, (PARAMS * tok_rows, PARAMS * tok_rows), 1)
    swap = jnp.where(ec == (er % PARAMS) * tok_rows + er // PARAMS, 1.0, 0.0).astype(BF16)
    table = mm(swap, stack, NN).astype(BF16)

    lane = lax.broadcasted_iota(jnp.int32, (8, 128), 1)
    mine_at = lax.rem(me, per)

    def gathered(buf):
        out = []
        for i in range(packs):
            total = None
            for k in range(per):
                q = lax.rem(mine_at + k, per)
                block = buf[i * per + q]
                if k:
                    block = pltpu.roll(block, k * cap, 1)
                total = block if total is None else jnp.where(lane // cap == q, block, total)
            out.append(total)
        return jnp.concatenate(out, axis=1)

    all_small(0, wanted).wait_recv()
    asks_in = gathered(wanted)
    ask_g = asks_in[1:2]
    ask_t = asks_in[0:1]
    hot = jnp.where(
        lax.broadcasted_iota(jnp.int32, (gpt, group * cap), 0) == ask_g.astype(jnp.int32), 1.0, 0.0
    ).astype(BF16)
    spread_rows = mm(table, hot, NN)
    answer = jnp.zeros((PARAMS, group * cap), F32)
    for t in range(tok_rows):
        answer = jnp.where(
            ask_t == float(t), spread_rows[t * PARAMS : (t + 1) * PARAMS], answer
        )
    for i in range(packs):
        found[i] = answer[:, i * 128 : (i + 1) * 128]
    given[me] = found[me // per]

    @pl.loop(1, group)
    def _(i):
        j, to = peer(i)
        small(2, found.at[j // per], given.at[me], to).start()

    norm_copy(0, pl.ds(0, nhi - 1), partner).wait_recv()
    for n, (s, l) in enumerate(beside + below):
        norm_copy(1 + n, line, (s, hi * nlo + l, scene)).start()

    all_small(1, lists).wait_recv()
    row_at = lax.broadcasted_iota(jnp.int32, (tokens, K), 0)
    gauss_at = lax.broadcasted_iota(jnp.int32, (gpt, K), 0)

    @pl.loop(0, group)
    def _(j):
        for b in range(tiles):
            cut = slice(b * K, (b + 1) * K)
            at = lists[j, pl.ds(b, 1), :]
            if ahead:
                where[j, :, cut] = jnp.where(row_at == at, 1.0, 0.0).astype(BF16)
            g = lists[j, pl.ds(tiles + b, 1), :]
            fits[j, :, cut] = jnp.where(gauss_at == g, 1.0, 0.0).astype(BF16)

    all_small(2, given).wait_recv()
    picked = mm(gathered(given).astype(BF16), perm[...], NN)
    rows = [picked[p : p + 1] for p in range(PARAMS)]
    loads[4].wait()

    place = lax.broadcasted_iota(jnp.int32, (1, pix), 1)
    across = ((place % SIDE).astype(F32) + 0.5) * (2.0 / SIDE) - 1.0
    down = ((place // SIDE).astype(F32) + 0.5) * (2.0 / SIDE) - 1.0
    ka = lax.broadcasted_iota(jnp.int32, (K, K), 0)
    kb = lax.broadcasted_iota(jnp.int32, (K, K), 1)
    lower = jnp.where(kb < ka, 1.0, 0.0).astype(BF16)
    upper = jnp.where(kb > ka, 1.0, 0.0).astype(BF16)
    ones = jnp.ones((8, pix), BF16)
    per_view = (tiles * group) // VIEWS
    slot = lax.broadcasted_iota(jnp.int32, (1, K), 1)
    loss_part = jnp.zeros((1, K), F32)
    outs = []

    for b in range(tiles):
        cut = slice(b * K, (b + 1) * K)
        mx, my, mz, ls, op, cr, cg, cb = [r[:, cut] for r in rows]
        vi = (me * tiles + b) // per_view
        cam = [cam_ref[vi, n] for n in range(8)]
        live = jnp.where(slot < count_ref[b], 1.0, 0.0)
        sx = jnp.tanh(cam[0] * mx + cam[1] * my + cam[2] * mz + cam[3])
        sy = jnp.tanh(cam[4] * mx + cam[5] * my + cam[6] * mz + cam[7])
        spread = jnp.exp(-2.0 * ls)
        sop = sigmoid(op)
        amp = 0.3 * sop * live
        shade = sigmoid(jnp.concatenate([cr, cg, cb], axis=0))
        shade8 = jnp.concatenate([shade, jnp.zeros((5, K), F32)], axis=0)
        cols = jnp.concatenate([sx, sy, spread, amp, jnp.zeros((K - 4, K), F32)], axis=0).T
        csx, csy, csp, camp = [cols[:, n : n + 1] for n in range(4)]
        dx = across - csx
        dy = down - csy
        r2 = dx * dx + dy * dy
        alpha = camp * jnp.exp(-0.5 * r2 * csp)
        rest = 1.0 - alpha
        trans = jnp.exp(mm2(lower, jnp.log(rest), NN))
        weight = alpha * trans
        colour = mm3(shade8, weight, NN)
        for c in range(3):
            image_ref[pl.ds(b, 1), c * pix : (c + 1) * pix] = colour[c : c + 1].astype(BF16)
        want = jnp.concatenate(
            [want_ref[pl.ds(b, 1), c * pix : (c + 1) * pix].astype(F32) for c in range(3)]
            + [jnp.zeros((5, pix), F32)],
            axis=0,
        )
        diff = colour - want
        sq = jnp.sum(diff * diff, axis=0, keepdims=True)
        part = sq[:, :K]
        for n in range(1, pix // K):
            part = part + sq[:, n * K : (n + 1) * K]
        loss_part = loss_part + part * factor
        dcol = (2.0 * factor) * diff
        dw = mm3(shade8, dcol, TN)
        dshade = mm3(dcol, weight, NT)
        dww = dw * weight
        dlogs = mm2(upper, dww, NN)
        h = dww - dlogs * alpha / rest
        s_h = mm2(ones, h, NT)[0:1]
        s_x = mm2(ones, h * dx, NT)[0:1]
        s_y = mm2(ones, h * dy, NT)[0:1]
        s_r = mm2(ones, h * r2, NT)[0:1]
        px = spread * s_x * (1.0 - sx * sx)
        py = spread * s_y * (1.0 - sy * sy)
        dcolour = dshade[0:3] * shade * (1.0 - shade)
        outs.append(
            jnp.concatenate(
                [
                    cam[0] * px + cam[4] * py,
                    cam[1] * px + cam[5] * py,
                    cam[2] * px + cam[6] * py,
                    spread * s_r,
                    (1.0 - sop) * s_h,
                    dcolour,
                ],
                axis=0,
            )
        )
    half = tiles // 2
    grads[me] = jnp.concatenate(
        [jnp.concatenate(outs[:half], axis=1), jnp.concatenate(outs[half:], axis=1)], axis=0
    ).astype(BF16)
    losses[me] = loss_part

    def push(n, buf, i, recv):
        j, to = peer(i)
        return pltpu.make_async_remote_copy(
            src_ref=buf.at[me], dst_ref=buf.at[me], send_sem=s_grad.at[n],
            recv_sem=recv, device_id=to, device_id_type=MESH,
        )

    @pl.loop(1, group)
    def _(i):
        push(0, grads, i, r_grad.at[me]).start()

    @pl.loop(1, group)
    def _(i):
        push(1, losses, i, s_loss.at[1]).start()

    nb = nsec - 1
    ns = nlo - 1
    for n in range(nb + ns):
        norm_copy(1 + n, line, partner).wait_recv()
    cut_rows = tok_rows // 2
    far = []
    for a, (s, _) in enumerate(beside):
        for b, (_, l) in enumerate(below):
            far.append((a, b, s, l))

    def far_copies():
        out = []
        base = 1 + nb + ns
        for m, (a, b, s, l) in enumerate(far):
            down_line = pl.ds((sec * nlo + l) * nhi, nhi)
            side_line = pl.ds((s * nlo + lo) * nhi, nhi)
            first = pl.ds(0, cut_rows)
            second = pl.ds(cut_rows, tok_rows - cut_rows)
            for n, span, part, to in (
                (base + 2 * m, down_line, first, (s, hi * nlo + lo, scene)),
                (base + 2 * m + 1, side_line, second, (sec, hi * nlo + l, scene)),
            ):
                out.append(
                    pltpu.make_async_remote_copy(
                        src_ref=norms.at[span, part], dst_ref=norms.at[span, part],
                        send_sem=s_norm.at[n], recv_sem=r_norm.at[n], device_id=to,
                        device_id_type=MESH,
                    )
                )
        return out

    for copy in far_copies():
        copy.start()

    @pl.loop(0, group)
    def _(i):
        j = peer(i)[0]

        @pl.when(i > 0)
        def _():
            push(0, grads, i, r_grad.at[j]).wait_recv()

        got = grads[j]
        fit = fits[j]
        wide = half * K
        spreadout = jnp.concatenate(
            [
                jnp.concatenate(
                    [
                        fit[:, :wide] * got[p : p + 1],
                        fit[:, wide:] * got[PARAMS + p : PARAMS + p + 1],
                    ],
                    axis=1,
                )
                for p in range(PARAMS)
            ],
            axis=0,
        )
        if not ahead:
            for b in range(tiles):
                at = lists[j, pl.ds(b, 1), :]
                where[0, :, b * K : (b + 1) * K] = jnp.where(row_at == at, 1.0, 0.0).astype(BF16)
        part = mm(where[j if ahead else 0], spreadout, NT)

        @pl.when(i == 0)
        def _():
            dhead[...] = part

        @pl.when(i > 0)
        def _():
            dhead[...] += part

    loss_all = losses.at[pl.ds(0, group - 1)]
    pltpu.make_async_remote_copy(
        src_ref=loss_all, dst_ref=loss_all, send_sem=s_grad.at[1], recv_sem=s_loss.at[1],
        device_id=partner, device_id_type=MESH,
    ).wait_recv()
    loss_mine[...] = jnp.broadcast_to(jnp.sum(losses[...], axis=0), loss_mine.shape)
    for copy in far_copies():
        copy.wait_recv()
    loss_copy = pltpu.make_async_remote_copy(
        src_ref=loss_mine, dst_ref=loss_theirs, send_sem=s_loss.at[0], recv_sem=r_loss,
        device_id=partner, device_id_type=MESH,
    )
    dh = dhead[...].astype(BF16)
    dhead_rows = 256
    chunks = width // dhead_rows

    def part_copy(n):
        span = pl.ds(n * dhead_rows, dhead_rows)
        return pltpu.make_async_remote_copy(
            src_ref=mine.at[span], dst_ref=theirs.at[span],
            send_sem=s_part.at[n], recv_sem=r_part.at[n],
            device_id=partner, device_id_type=MESH,
        )

    for n in range(chunks):
        a = norms[:, :, n * dhead_rows : (n + 1) * dhead_rows].reshape(tokens, dhead_rows)
        mine[n * dhead_rows : (n + 1) * dhead_rows, :] = mm(a, dh, TN).astype(BF16)
        if n == 0:
            loss_copy.start()
        else:
            part_copy(n - 1).start()
    part_copy(chunks - 1).start()

    for n in range(chunks):
        part_copy(n).wait_recv()
        span = slice(n * dhead_rows, (n + 1) * dhead_rows)
        grad_ref[span, :] = (mine[span, :].astype(F32) + theirs[span, :].astype(F32)).astype(BF16)
    loss_copy.wait_recv()
    loss_ref[...] = jnp.broadcast_to(
        jnp.sum(loss_mine[0:1] + loss_theirs[0:1], keepdims=True), loss_ref.shape
    )

    loss_copy.wait_send()
    for n in range(chunks):
        part_copy(n).wait_send()
    all_small(0, wanted).wait_send()
    all_small(1, lists).wait_send()
    all_small(2, given).wait_send()
    grad_all = grads.at[pl.ds(0, group - 1)]
    pltpu.make_async_remote_copy(
        src_ref=grad_all, dst_ref=grad_all, send_sem=s_grad.at[0], recv_sem=r_grad.at[0],
        device_id=partner, device_id_type=MESH,
    ).wait_send()
    pltpu.make_async_remote_copy(
        src_ref=loss_all, dst_ref=loss_all, send_sem=s_grad.at[1], recv_sem=s_loss.at[1],
        device_id=partner, device_id_type=MESH,
    ).wait_send()
    norm_copy(0, pl.ds(0, nhi - 1), partner).wait_send()
    for n in range(nb + ns):
        norm_copy(1 + n, line, partner).wait_send()
    for copy in far_copies():
        copy.wait_send()


def solution(mesh):
    nsec, nview, nscene = mesh.shape["section"], mesh.shape["view"], mesh.shape["scene"]
    group = nsec * nview
    nlo = 2 if nview % 2 == 0 else 1

    def body(tokens, norm_gain, head_weight, tile_lists, tile_counts, cameras, targets):
        tok_rows, width = tokens.shape[1:]
        outw = head_weight.shape[1]
        gpt = outw // PARAMS
        tiles, K = tile_lists.shape[1:]
        slots = tiles * K
        cap = 2 * slots // group
        packs = group * cap // 128
        factor = 1.0 / (nscene * tiles * group)
        ahead = group * group * tok_rows * slots <= 2**24
        flows = 1 + (nsec - 1) + (nlo - 1) + 2 * (nsec - 1) * (nlo - 1)
        vmem = pl.BlockSpec(memory_space=pltpu.VMEM)
        smem = pl.BlockSpec(memory_space=pltpu.SMEM)
        hbm = pl.BlockSpec(memory_space=pl.ANY)
        dma = pltpu.SemaphoreType.DMA
        image, grad, loss = pl.pallas_call(
            functools.partial(kernel, nsec, nview, factor),
            out_shape=(
                jax.ShapeDtypeStruct((tiles, targets.shape[2]), BF16),
                jax.ShapeDtypeStruct((width, outw), BF16),
                jax.ShapeDtypeStruct((8, 128), F32),
            ),
            in_specs=[hbm, hbm, hbm, hbm, smem, smem, hbm],
            out_specs=(vmem, vmem, vmem),
            scratch_shapes=[
                pltpu.VMEM((tok_rows, width), BF16),
                pltpu.VMEM((1, width), F32),
                pltpu.VMEM((width, outw), BF16),
                pltpu.VMEM((tiles, K), jnp.int32),
                pltpu.VMEM((tiles, targets.shape[2]), BF16),
                pltpu.VMEM((group * cap, slots), BF16),
                pltpu.VMEM((packs, 8, 128), F32),
                pltpu.VMEM((group, 8, 128), F32),
                pltpu.VMEM((packs, 8, 128), F32),
                pltpu.VMEM((group, 8, 128), F32),
                pltpu.VMEM((group, 2 * tiles, K), jnp.int32),
                pltpu.VMEM((group if ahead else 1, group * tok_rows, slots), BF16),
                pltpu.VMEM((group, gpt, slots), BF16),
                pltpu.VMEM((group, tok_rows, width), BF16),
                pltpu.VMEM((group, 2 * PARAMS, slots // 2), BF16),
                pltpu.VMEM((group * tok_rows, outw), F32),
                pltpu.VMEM((width, outw), BF16),
                pltpu.VMEM((width, outw), BF16),
                pltpu.VMEM((group, 1, K), F32),
                pltpu.VMEM((8, K), F32),
                pltpu.VMEM((8, K), F32),
                dma((5,)),
                dma((3,)), dma((3,)),
                dma((flows,)), dma((flows,)),
                dma((2,)), dma((group,)),
                dma((width // 256,)), dma((width // 256,)),
                dma((2,)), dma,
            ],
            compiler_params=pltpu.CompilerParams(
                collective_id=0, has_side_effects=True, vmem_limit_bytes=60 * 1024 * 1024
            ),
        )(
            tokens[0], norm_gain[None], head_weight, tile_lists[0], tile_counts[0], cameras[0],
            targets[0],
        )
        return image[None], grad.astype(F32), loss[0, 0]

    in_specs = (
        P("scene", ("section", "view"), None),
        P(),
        P(),
        P("scene", ("section", "view"), None),
        P("scene", ("section", "view")),
        P("scene", None, None),
        P("scene", ("section", "view"), None),
    )
    out_specs = (P("scene", ("section", "view"), None), P(), P())
    return jax.shard_map(body, mesh=mesh, in_specs=in_specs, out_specs=out_specs, check_vma=False)
```

```python
import functools

import jax
import jax.numpy as jnp
from jax import lax
from jax.experimental import pallas as pl
from jax.experimental.pallas import tpu as pltpu
from jax.sharding import PartitionSpec as P

PARAMS = 8
SIDE = 16
BATCH = 4
VIEWS = 2
MESH = pl.DeviceIdType.MESH
F32 = jnp.float32
BF16 = jnp.bfloat16
LOG2E = 1.4426950408889634
NN = (((1,), (0,)), ((), ()))
NT = (((1,), (1,)), ((), ()))
TN = (((0,), (0,)), ((), ()))


def mm(a, b, dims):
    return lax.dot_general(a, b, dims, preferred_element_type=F32)


def split(x):
    hi = x.astype(BF16)
    lo = (x - hi.astype(F32)).astype(BF16)
    return hi, lo


def sigmoid(x):
    return 1.0 / (1.0 + jnp.exp(-x))


def turn(a, k, n):
    if n & (n - 1):
        return lax.rem(a + k, n)
    out, bit = 0, 1
    while bit < n:
        out = out + bit * lax.rem((a // bit) + (k // bit), 2)
        bit *= 2
    return out


def kernel(
    nsec, nview, factor,
    tok_hbm, gain_hbm, w_hbm, list_hbm, count_ref, cam_ref, want_hbm,
    image_ref, grad_ref, loss_ref,
    tok_ref, gain_ref, w_ref, list_ref, want_ref,
    perm, asked, wanted, found, given, lists, where, fits, norms, grads, dhead, turned, mine, theirs,
    losses, loss_mine, loss_theirs,
    s_in, s_small, r_small, s_norm, r_norm, s_grad, r_grad, s_part, r_part, s_loss, r_loss,
):
    group = nsec * nview
    nlo = 2 if nview % 2 == 0 else 1
    nhi = nview // nlo
    sec, view, scene = lax.axis_index("section"), lax.axis_index("view"), lax.axis_index("scene")
    hi, lo = view // nlo, lax.rem(view, nlo)
    me = sec * nview + view
    tok_rows, width = tok_ref.shape
    outw = w_ref.shape[1]
    gpt = outw // PARAMS
    tiles, K = list_ref.shape
    slots = tiles * K
    tokens = group * tok_rows
    pix = SIDE * SIDE
    cap = 2 * slots // group
    per = 128 // cap
    packs = group // per
    ahead = where.shape[0] > 1
    batch = where.shape[2] // slots

    def local(n, src, dst):
        return pltpu.make_async_copy(src, dst, s_in.at[n])

    loads = [
        local(0, list_hbm, list_ref),
        local(1, tok_hbm, tok_ref),
        local(2, gain_hbm, gain_ref),
        local(3, w_hbm, w_ref),
        local(4, want_hbm, want_ref),
    ]
    for load in loads:
        load.start()

    def peer(i):
        s = turn(sec, lax.rem(i, nsec), nsec)
        l = turn(lo, lax.rem(i // nsec, nlo), nlo)
        h = turn(hi, i // (nsec * nlo), nhi)
        v = h * nlo + l
        return s * nview + v, (s, v, scene)

    def place_of(s, l, h):
        return (s * nlo + l) * nhi + h

    partner = (sec, view, 1 - scene)
    barrier = pltpu.get_barrier_semaphore()

    @pl.loop(1, group)
    def _(i):
        pl.semaphore_signal(barrier, inc=1, device_id=peer(i)[1], device_id_type=MESH)

    pl.semaphore_signal(barrier, inc=1, device_id=partner, device_id_type=MESH)

    loads[0].wait()
    number = jnp.concatenate([list_ref[pl.ds(b, 1), :] for b in range(tiles)], axis=1)
    token = number // gpt
    gauss = number - token * gpt
    owner = token // tok_rows
    inner = token - owner * tok_rows
    ow_sec = owner // nview
    ow_hi = (owner - ow_sec * nview) // nlo
    ow_lo = owner - ow_sec * nview - ow_hi * nlo
    row = place_of(ow_sec, ow_lo, ow_hi) * tok_rows + inner
    for b in range(tiles):
        cut = slice(b * K, (b + 1) * K)
        lists[me, pl.ds(b, 1), :] = row[:, cut]
        lists[me, pl.ds(tiles + b, 1), :] = gauss[:, cut]
    mask = jnp.where(lax.broadcasted_iota(jnp.int32, (group, slots), 0) == owner, 1.0, 0.0)
    earlier = jnp.where(
        lax.broadcasted_iota(jnp.int32, (slots, slots), 0)
        < lax.broadcasted_iota(jnp.int32, (slots, slots), 1),
        1.0, 0.0,
    ).astype(BF16)
    rank = jnp.sum(mask * mm(mask.astype(BF16), earlier, NN), axis=0, keepdims=True)
    dest = owner * cap + rank.astype(jnp.int32)
    perm[...] = jnp.where(
        lax.broadcasted_iota(jnp.int32, (group * cap, slots), 0) == dest, 1.0, 0.0
    ).astype(BF16)
    asks = jnp.concatenate(
        [inner.astype(F32), gauss.astype(F32), jnp.zeros((6, slots), F32)], axis=0
    ).astype(BF16)
    requests = mm(asks, perm[...], NT)
    for i in range(packs):
        asked[i] = requests[:, i * 128 : (i + 1) * 128]
    wanted[me] = asked[me // per]

    pl.semaphore_wait(barrier, group)

    def small(n, src, dst, where_to):
        return pltpu.make_async_remote_copy(
            src_ref=src, dst_ref=dst, send_sem=s_small.at[n], recv_sem=r_small.at[n],
            device_id=where_to, device_id_type=MESH,
        )

    def all_small(n, buf):
        span = buf.at[pl.ds(0, group - 1)]
        return small(n, span, span, partner)

    @pl.loop(1, group)
    def _(i):
        j, to = peer(i)
        small(0, asked.at[j // per], wanted.at[me], to).start()

    @pl.loop(1, group)
    def _(i):
        small(1, lists.at[me], lists.at[me], peer(i)[1]).start()

    loads[1].wait()
    loads[2].wait()
    spot = place_of(sec, lo, hi)
    x = tok_ref[...].astype(F32)
    scale = lax.rsqrt(jnp.mean(x * x, axis=-1, keepdims=True) + 1e-06)
    normed = (x * scale * gain_ref[...]).astype(BF16)
    norms[spot] = normed

    def norm_copy(n, span, to):
        return pltpu.make_async_remote_copy(
            src_ref=norms.at[span], dst_ref=norms.at[span], send_sem=s_norm.at[n],
            recv_sem=r_norm.at[n], device_id=to, device_id_type=MESH,
        )

    def line_copy(k):
        h = turn(hi, k, nhi)
        return norm_copy(0, pl.ds(spot, 1), (sec, h * nlo + lo, scene))

    line = pl.ds((sec * nlo + lo) * nhi, nhi)
    beside = [(turn(sec, k, nsec), lo) for k in range(1, nsec)]
    below = [(sec, turn(lo, k, nlo)) for k in range(1, nlo)]

    @pl.loop(1, nhi)
    def _(k):
        line_copy(k).start()

    loads[3].wait()
    head = mm(normed, w_ref[...], NN)
    stack = jnp.concatenate(
        [head[:, p * gpt : (p + 1) * gpt] for p in range(PARAMS)], axis=0
    ).astype(BF16)
    er = lax.broadcasted_iota(jnp.int32, (PARAMS * tok_rows, PARAMS * tok_rows), 0)
    ec = lax.broadcasted_iota(jnp.int32, (PARAMS * tok_rows, PARAMS * tok_rows), 1)
    swap = jnp.where(ec == (er % PARAMS) * tok_rows + er // PARAMS, 1.0, 0.0).astype(BF16)
    table = mm(swap, stack, NN).astype(BF16)

    lane = lax.broadcasted_iota(jnp.int32, (8, 128), 1)
    mine_at = lax.rem(me, per)

    def gathered(buf):
        out = []
        for i in range(packs):
            total = None
            for k in range(per):
                q = lax.rem(mine_at + k, per)
                block = buf[i * per + q]
                if k:
                    block = pltpu.roll(block, k * cap, 1)
                total = block if total is None else jnp.where(lane // cap == q, block, total)
            out.append(total)
        return jnp.concatenate(out, axis=1)

    all_small(0, wanted).wait_recv()
    asks_in = gathered(wanted)
    ask_g = asks_in[1:2]
    ask_t = asks_in[0:1]
    hot = jnp.where(
        lax.broadcasted_iota(jnp.int32, (gpt, group * cap), 0) == ask_g.astype(jnp.int32), 1.0, 0.0
    ).astype(BF16)
    spread_rows = mm(table, hot, NN)
    answer = jnp.zeros((PARAMS, group * cap), F32)
    for t in range(tok_rows):
        answer = jnp.where(
            ask_t == float(t), spread_rows[t * PARAMS : (t + 1) * PARAMS], answer
        )
    for i in range(packs):
        found[i] = answer[:, i * 128 : (i + 1) * 128]
    given[me] = found[me // per]

    @pl.loop(1, group)
    def _(i):
        j, to = peer(i)
        small(2, found.at[j // per], given.at[me], to).start()

    norm_copy(0, pl.ds(0, nhi - 1), partner).wait_recv()
    for n, (s, l) in enumerate(beside + below):
        norm_copy(1 + n, line, (s, hi * nlo + l, scene)).start()
    stretch = nhi * tok_rows

    def turn_line(n):
        block = norms[n * nhi : (n + 1) * nhi].reshape(stretch, width)
        turned[:, n * stretch : (n + 1) * stretch] = block.T

    all_small(1, lists).wait_recv()
    row_at = lax.broadcasted_iota(jnp.int32, (tokens, K), 0)
    gauss_at = lax.broadcasted_iota(jnp.int32, (gpt, K), 0)

    def mark_rows(g, n):
        for q in range(batch):
            j = peer(g * batch + q)[0]
            for b in range(tiles):
                at = lists[j, pl.ds(b, 1), :]
                where[n, :, (q * tiles + b) * K : (q * tiles + b + 1) * K] = jnp.where(
                    row_at == at, 1.0, 0.0
                ).astype(BF16)

    @pl.loop(0, group // batch)
    def _(g):
        if ahead:
            mark_rows(g, g)

    @pl.loop(0, group)
    def _(j):
        for b in range(tiles):
            at = lists[j, pl.ds(tiles + b, 1), :]
            fits[j, :, b * K : (b + 1) * K] = jnp.where(gauss_at == at, 1.0, 0.0).astype(BF16)

    all_small(2, given).wait_recv()
    picked = mm(gathered(given).astype(BF16), perm[...], NN)
    rows = [picked[p : p + 1] for p in range(PARAMS)]
    loads[4].wait()

    place = lax.broadcasted_iota(jnp.int32, (1, pix), 1)
    across = ((place % SIDE).astype(F32) + 0.5) * (2.0 / SIDE) - 1.0
    down = ((place // SIDE).astype(F32) + 0.5) * (2.0 / SIDE) - 1.0
    ka = lax.broadcasted_iota(jnp.int32, (K, 2 * K), 0)
    kb = lax.rem(lax.broadcasted_iota(jnp.int32, (K, 2 * K), 1), K)
    lower = jnp.where(kb < ka, 1.0, 0.0).astype(BF16)
    upper = jnp.where(kb > ka, 1.0, 0.0).astype(BF16)
    moments = jnp.concatenate(
        [jnp.ones((1, pix), F32), across, down, across * across + down * down, jnp.zeros((4, pix), F32)],
        axis=0,
    ).astype(BF16)
    vi = me * VIEWS // group
    cam = [cam_ref[vi, n] for n in range(8)]
    slot = lax.broadcasted_iota(jnp.int32, (1, K), 1)
    live = jnp.concatenate(
        [jnp.where(slot < count_ref[b], 1.0, 0.0) for b in range(tiles)], axis=1
    )
    mx, my, mz, ls, op = rows[:5]
    sx = jnp.tanh(cam[0] * mx + cam[1] * my + cam[2] * mz + cam[3])
    sy = jnp.tanh(cam[4] * mx + cam[5] * my + cam[6] * mz + cam[7])
    spread = jnp.exp(-2.0 * ls)
    sop = sigmoid(op)
    amp = 0.3 * sop * live
    shade = sigmoid(picked[5:8])
    shade8 = jnp.concatenate([shade, jnp.zeros((5, slots), F32)], axis=0)
    steep = (-0.5 * LOG2E) * jnp.minimum(spread, 1e38)
    cols = jnp.concatenate([sx, sy, steep, amp, jnp.zeros((4, slots), F32)], axis=0).T
    cuts = [slice(b * K, (b + 1) * K) for b in range(tiles)]

    alphas, inverses, logs = [], [], []
    for cut in cuts:
        csx, csy, csp, camp = [cols[cut, n : n + 1] for n in range(4)]
        dx = across - csx
        dy = down - csy
        alpha = camp * jnp.exp2((dx * dx + dy * dy) * csp)
        rest = 1.0 - alpha
        alphas.append(alpha)
        inverses.append(alpha / rest)
        logs.append(jnp.concatenate(split(jnp.log(rest)), axis=0))
    befores = [mm(lower, x, NN) for x in logs]
    weights = [alpha * jnp.exp(before) for alpha, before in zip(alphas, befores)]
    packed = [weight.astype(BF16) for weight in weights]
    shade_hi, shade_lo = split(shade8)
    shade_two = jnp.concatenate([shade_hi, shade_lo], axis=0)
    colours = []
    for cut, weight in zip(cuts, packed):
        both = mm(shade_two[:, cut], weight, NN)
        colours.append(both[:8] + both[8:])
    loss_part = jnp.zeros((1, K), F32)
    dcols = []
    for b in range(tiles):
        want = jnp.concatenate(
            [want_ref[pl.ds(b, 1), c * pix : (c + 1) * pix].astype(F32) for c in range(3)]
            + [jnp.zeros((5, pix), F32)],
            axis=0,
        )
        for c in range(3):
            image_ref[pl.ds(b, 1), c * pix : (c + 1) * pix] = colours[b][c : c + 1].astype(BF16)
        diff = colours[b] - want
        sq = jnp.sum(diff * diff, axis=0, keepdims=True)
        for n in range(0, pix, K):
            loss_part = loss_part + sq[:, n : n + K]
        dcols.append(((2.0 * factor) * diff).astype(BF16))
    losses[me] = loss_part * factor
    dshade = jnp.concatenate([mm(d, w, NT) for d, w in zip(dcols, packed)], axis=1)
    dwws = [
        mm(shade_hi[:, cut], d, TN) * weight for cut, d, weight in zip(cuts, dcols, weights)
    ]
    dlogs = [mm(upper[:, :K], x.astype(BF16), NN) for x in dwws]
    sums = []
    for x, y, inverse in zip(dwws, dlogs, inverses):
        h = x - y * inverse
        both = mm(moments, jnp.concatenate(split(h), axis=0), NT)
        sums.append(both[:, :K] + both[:, K:])
    sums = jnp.concatenate(sums, axis=1)
    s_h, s_u, s_v, s_q = [sums[n : n + 1] for n in range(4)]
    s_x = s_u - sx * s_h
    s_y = s_v - sy * s_h
    s_r = s_q - 2.0 * (sx * s_u + sy * s_v) + (sx * sx + sy * sy) * s_h
    px = spread * s_x * (1.0 - sx * sx)
    py = spread * s_y * (1.0 - sy * sy)
    out = jnp.concatenate(
        [
            cam[0] * px + cam[4] * py,
            cam[1] * px + cam[5] * py,
            cam[2] * px + cam[6] * py,
            spread * s_r,
            (1.0 - sop) * s_h,
            dshade[0:3] * shade * (1.0 - shade),
        ],
        axis=0,
    )
    wide = slots // 2
    grads[me] = jnp.concatenate([out[:, :wide], out[:, wide:]], axis=0).astype(BF16)

    def push(n, buf, i, recv):
        j, to = peer(i)
        return pltpu.make_async_remote_copy(
            src_ref=buf.at[me], dst_ref=buf.at[me], send_sem=s_grad.at[n],
            recv_sem=recv, device_id=to, device_id_type=MESH,
        )

    @pl.loop(1, group)
    def _(i):
        push(0, grads, i, r_grad.at[me]).start()

    @pl.loop(1, group)
    def _(i):
        push(1, losses, i, s_loss.at[1]).start()

    nb = nsec - 1
    ns = nlo - 1
    for n in range(nb + ns):
        norm_copy(1 + n, line, partner).wait_recv()
    cut_rows = tok_rows // 2
    far = []
    for a, (s, _) in enumerate(beside):
        for b, (_, l) in enumerate(below):
            far.append((a, b, s, l))

    def far_copies():
        out = []
        base = 1 + nb + ns
        for m, (a, b, s, l) in enumerate(far):
            down_line = pl.ds((sec * nlo + l) * nhi, nhi)
            side_line = pl.ds((s * nlo + lo) * nhi, nhi)
            first = pl.ds(0, cut_rows)
            second = pl.ds(cut_rows, tok_rows - cut_rows)
            for n, span, part, to in (
                (base + 2 * m, down_line, first, (s, hi * nlo + lo, scene)),
                (base + 2 * m + 1, side_line, second, (sec, hi * nlo + l, scene)),
            ):
                out.append(
                    pltpu.make_async_remote_copy(
                        src_ref=norms.at[span, part], dst_ref=norms.at[span, part],
                        send_sem=s_norm.at[n], recv_sem=r_norm.at[n], device_id=to,
                        device_id_type=MESH,
                    )
                )
        return out

    for copy in far_copies():
        copy.start()

    def gather_batch(g, n):
        sides = []
        for q in range(batch):
            i = g * batch + q
            j = peer(i)[0]
            if isinstance(i, int):
                if i > 0:
                    push(0, grads, i, r_grad.at[j]).wait_recv()
            else:
                pl.when(i > 0)(lambda: push(0, grads, i, r_grad.at[j]).wait_recv())
            got = grads[j]
            fit = fits[j]
            sides.append(
                jnp.concatenate(
                    [
                        jnp.concatenate(
                            [
                                fit[:, :wide] * got[p : p + 1],
                                fit[:, wide:] * got[PARAMS + p : PARAMS + p + 1],
                            ],
                            axis=1,
                        )
                        for p in range(PARAMS)
                    ],
                    axis=0,
                )
            )
        return mm(jnp.concatenate(sides, axis=1), where[n], NT)

    if ahead:
        dhead[...] = gather_batch(0, 0)
        for g in range(1, group // batch):
            dhead[...] += gather_batch(g, g)
    else:
        dhead[...] = jnp.zeros_like(dhead)

        @pl.loop(0, group // batch)
        def _(g):
            mark_rows(g, 0)
            dhead[...] += gather_batch(g, 0)

    loss_all = losses.at[pl.ds(0, group - 1)]
    pltpu.make_async_remote_copy(
        src_ref=loss_all, dst_ref=loss_all, send_sem=s_grad.at[1], recv_sem=s_loss.at[1],
        device_id=partner, device_id_type=MESH,
    ).wait_recv()
    loss_mine[...] = jnp.broadcast_to(jnp.sum(losses[...], axis=0), loss_mine.shape)
    for copy in far_copies():
        copy.wait_recv()
    loss_copy = pltpu.make_async_remote_copy(
        src_ref=loss_mine, dst_ref=loss_theirs, send_sem=s_loss.at[0], recv_sem=r_loss,
        device_id=partner, device_id_type=MESH,
    )
    for n in range(nsec * nlo):
        turn_line(n)
    dh = dhead[...].astype(BF16)
    dhead_rows = 256
    chunks = width // dhead_rows

    def part_copy(n):
        span = pl.ds(n * dhead_rows, dhead_rows)
        return pltpu.make_async_remote_copy(
            src_ref=mine.at[span], dst_ref=theirs.at[span],
            send_sem=s_part.at[n], recv_sem=r_part.at[n],
            device_id=partner, device_id_type=MESH,
        )

    for n in range(chunks):
        span = slice(n * dhead_rows, (n + 1) * dhead_rows)
        mine[span, :] = mm(turned[span, :], dh, NT).astype(BF16)
        if n == 0:
            loss_copy.start()
        else:
            part_copy(n - 1).start()
    part_copy(chunks - 1).start()

    for n in range(chunks):
        part_copy(n).wait_recv()
        span = slice(n * dhead_rows, (n + 1) * dhead_rows)
        grad_ref[span, :] = (mine[span, :].astype(F32) + theirs[span, :].astype(F32)).astype(BF16)
    loss_copy.wait_recv()
    loss_ref[...] = jnp.broadcast_to(
        jnp.sum(loss_mine[0:1] + loss_theirs[0:1], keepdims=True), loss_ref.shape
    )

    loss_copy.wait_send()
    for n in range(chunks):
        part_copy(n).wait_send()
    all_small(0, wanted).wait_send()
    all_small(1, lists).wait_send()
    all_small(2, given).wait_send()
    grad_all = grads.at[pl.ds(0, group - 1)]
    pltpu.make_async_remote_copy(
        src_ref=grad_all, dst_ref=grad_all, send_sem=s_grad.at[0], recv_sem=r_grad.at[0],
        device_id=partner, device_id_type=MESH,
    ).wait_send()
    pltpu.make_async_remote_copy(
        src_ref=loss_all, dst_ref=loss_all, send_sem=s_grad.at[1], recv_sem=s_loss.at[1],
        device_id=partner, device_id_type=MESH,
    ).wait_send()
    norm_copy(0, pl.ds(0, nhi - 1), partner).wait_send()
    for n in range(nb + ns):
        norm_copy(1 + n, line, partner).wait_send()
    for copy in far_copies():
        copy.wait_send()


def solution(mesh):
    nsec, nview, nscene = mesh.shape["section"], mesh.shape["view"], mesh.shape["scene"]
    group = nsec * nview
    nlo = 2 if nview % 2 == 0 else 1

    def body(tokens, norm_gain, head_weight, tile_lists, tile_counts, cameras, targets):
        tok_rows, width = tokens.shape[1:]
        outw = head_weight.shape[1]
        gpt = outw // PARAMS
        tiles, K = tile_lists.shape[1:]
        slots = tiles * K
        cap = 2 * slots // group
        packs = group * cap // 128
        factor = 1.0 / (nscene * tiles * group)
        ahead = group * group * tok_rows * slots <= 2**24
        batch = min(BATCH, group)
        flows = 1 + (nsec - 1) + (nlo - 1) + 2 * (nsec - 1) * (nlo - 1)
        vmem = pl.BlockSpec(memory_space=pltpu.VMEM)
        smem = pl.BlockSpec(memory_space=pltpu.SMEM)
        hbm = pl.BlockSpec(memory_space=pl.ANY)
        dma = pltpu.SemaphoreType.DMA
        image, grad, loss = pl.pallas_call(
            functools.partial(kernel, nsec, nview, factor),
            out_shape=(
                jax.ShapeDtypeStruct((tiles, targets.shape[2]), BF16),
                jax.ShapeDtypeStruct((width, outw), BF16),
                jax.ShapeDtypeStruct((8, 128), F32),
            ),
            in_specs=[hbm, hbm, hbm, hbm, smem, smem, hbm],
            out_specs=(vmem, vmem, vmem),
            scratch_shapes=[
                pltpu.VMEM((tok_rows, width), BF16),
                pltpu.VMEM((1, width), F32),
                pltpu.VMEM((width, outw), BF16),
                pltpu.VMEM((tiles, K), jnp.int32),
                pltpu.VMEM((tiles, targets.shape[2]), BF16),
                pltpu.VMEM((group * cap, slots), BF16),
                pltpu.VMEM((packs, 8, 128), F32),
                pltpu.VMEM((group, 8, 128), F32),
                pltpu.VMEM((packs, 8, 128), F32),
                pltpu.VMEM((group, 8, 128), F32),
                pltpu.VMEM((group, 2 * tiles, K), jnp.int32),
                pltpu.VMEM((group // batch if ahead else 1, group * tok_rows, batch * slots), BF16),
                pltpu.VMEM((group, gpt, slots), BF16),
                pltpu.VMEM((group, tok_rows, width), BF16),
                pltpu.VMEM((group, 2 * PARAMS, slots // 2), BF16),
                pltpu.VMEM((outw, group * tok_rows), F32),
                pltpu.VMEM((width, group * tok_rows), BF16),
                pltpu.VMEM((width, outw), BF16),
                pltpu.VMEM((width, outw), BF16),
                pltpu.VMEM((group, 1, K), F32),
                pltpu.VMEM((8, K), F32),
                pltpu.VMEM((8, K), F32),
                dma((5,)),
                dma((3,)), dma((3,)),
                dma((flows,)), dma((flows,)),
                dma((2,)), dma((group,)),
                dma((width // 256,)), dma((width // 256,)),
                dma((2,)), dma,
            ],
            compiler_params=pltpu.CompilerParams(
                collective_id=0, has_side_effects=True, vmem_limit_bytes=60 * 1024 * 1024
            ),
        )(
            tokens[0], norm_gain[None], head_weight, tile_lists[0], tile_counts[0], cameras[0],
            targets[0],
        )
        return image[None], grad.astype(F32), loss[0, 0]

    in_specs = (
        P("scene", ("section", "view"), None),
        P(),
        P(),
        P("scene", ("section", "view"), None),
        P("scene", ("section", "view")),
        P("scene", None, None),
        P("scene", ("section", "view"), None),
    )
    out_specs = (P("scene", ("section", "view"), None), P(), P())
    return jax.shard_map(body, mesh=mesh, in_specs=in_specs, out_specs=out_specs, check_vma=False)
```

```python
import functools

import jax
import jax.numpy as jnp
from jax import lax
from jax.experimental import pallas as pl
from jax.experimental.pallas import tpu as pltpu
from jax.sharding import PartitionSpec as P

PARAMS = 8
SIDE = 16
BATCH = 2
STORES = 1
LATE = 1
VIEWS = 2
MESH = pl.DeviceIdType.MESH
F32 = jnp.float32
BF16 = jnp.bfloat16
LOG2E = 1.4426950408889634
NN = (((1,), (0,)), ((), ()))
NT = (((1,), (1,)), ((), ()))
TN = (((0,), (0,)), ((), ()))


def mm(a, b, dims):
    return lax.dot_general(a, b, dims, preferred_element_type=F32)


def split(x):
    hi = x.astype(BF16)
    lo = (x - hi.astype(F32)).astype(BF16)
    return hi, lo


def sigmoid(x):
    return 1.0 / (1.0 + jnp.exp(-x))


def turn(a, k, n):
    if n & (n - 1):
        return lax.rem(a + k, n)
    if isinstance(k, int):
        bit = 1
        while bit < n:
            if k & bit:
                a = a + bit - 2 * bit * lax.rem(a // bit, 2)
            bit *= 2
        return a
    out, bit = 0, 1
    while bit < n:
        out = out + bit * lax.rem((a // bit) + (k // bit), 2)
        bit *= 2
    return out


def kernel(
    nsec, nview, factor,
    tok_hbm, gain_hbm, w_hbm, list_hbm, count_ref, cam_ref, want_hbm,
    image_ref, grad_ref, loss_ref,
    tok_ref, gain_ref, w_ref, list_ref, want_ref,
    perm, asked, wanted, found, given, lists, where, fits, norms, grads, dhead, turned, mine, theirs,
    losses, loss_mine, loss_theirs,
    s_in, s_small, r_small, s_norm, r_norm, s_grad, r_grad, s_part, r_part, s_loss, r_loss,
):
    group = nsec * nview
    nlo = 2
    nhi = nview // nlo
    sec, view, scene = lax.axis_index("section"), lax.axis_index("view"), lax.axis_index("scene")
    hi, lo = view // nlo, lax.rem(view, nlo)
    me = sec * nview + view
    tok_rows, width = tok_ref.shape
    outw = w_ref.shape[1]
    gpt = outw // PARAMS
    tiles, K = list_ref.shape
    slots = tiles * K
    tokens = group * tok_rows
    pix = SIDE * SIDE
    cap = 2 * slots // group
    per = 128 // cap
    packs = group // per
    ahead = where.shape[0] > 1
    batch = where.shape[2] // slots

    def local(n, src, dst):
        return pltpu.make_async_copy(src, dst, s_in.at[n])

    loads = [
        local(0, list_hbm, list_ref),
        local(1, tok_hbm, tok_ref),
        local(2, gain_hbm, gain_ref),
        local(3, w_hbm, w_ref),
        local(4, want_hbm, want_ref),
    ]
    for load in loads:
        load.start()

    known = {}

    def each_peer(act):
        if group <= 16:
            for i in range(group - 1, 0, -1):
                act(i)
        else:
            pl.loop(1, group)(act)

    def peer(i):
        if isinstance(i, int):
            if i not in known:
                known[i] = find(i)
            return known[i]
        return find(i)

    def find(i):
        s = turn(sec, i % nsec, nsec)
        l = turn(lo, (i // nsec) % nlo, nlo)
        h = turn(hi, i // (nsec * nlo), nhi)
        v = h * nlo + l
        return s * nview + v, (s, v, scene)

    def place_of(s, l, h):
        return (s * nlo + l) * nhi + h

    partner = (sec, view, 1 - scene)
    barrier = pltpu.get_barrier_semaphore()

    @each_peer
    def _(i):
        pl.semaphore_signal(barrier, inc=1, device_id=peer(i)[1], device_id_type=MESH)

    pl.semaphore_signal(barrier, inc=1, device_id=partner, device_id_type=MESH)

    loads[0].wait()
    number = jnp.concatenate([list_ref[pl.ds(b, 1), :] for b in range(tiles)], axis=1)
    token = number // gpt
    gauss = number - token * gpt
    owner = token // tok_rows
    inner = token - owner * tok_rows
    ow_sec = owner // nview
    ow_hi = (owner - ow_sec * nview) // nlo
    ow_lo = owner - ow_sec * nview - ow_hi * nlo
    row = place_of(ow_sec, ow_lo, ow_hi) * tok_rows + inner
    code = row * gpt + gauss
    for b in range(tiles):
        lists[me, pl.ds(b, 1), :] = code[:, b * K : (b + 1) * K]
    mask = jnp.where(lax.broadcasted_iota(jnp.int32, (group, slots), 0) == owner, 1.0, 0.0)
    earlier = jnp.where(
        lax.broadcasted_iota(jnp.int32, (slots, slots), 0)
        < lax.broadcasted_iota(jnp.int32, (slots, slots), 1),
        1.0, 0.0,
    ).astype(BF16)
    rank = jnp.sum(mask * mm(mask.astype(BF16), earlier, NN), axis=0, keepdims=True)
    dest = owner * cap + rank.astype(jnp.int32)
    perm[...] = jnp.where(
        lax.broadcasted_iota(jnp.int32, (group * cap, slots), 0) == dest, 1.0, 0.0
    ).astype(BF16)
    asks = jnp.concatenate(
        [inner.astype(F32), gauss.astype(F32), jnp.zeros((6, slots), F32)], axis=0
    ).astype(BF16)
    requests = mm(asks, perm[...], NT)
    requests = requests[0:1] * float(gpt) + requests[1:2]
    for i in range(packs):
        asked[i] = requests[:, i * 128 : (i + 1) * 128]
    wanted[me] = asked[me // per]

    pl.semaphore_wait(barrier, group)

    def small(n, src, dst, where_to):
        return pltpu.make_async_remote_copy(
            src_ref=src, dst_ref=dst, send_sem=s_small.at[n], recv_sem=r_small.at[n],
            device_id=where_to, device_id_type=MESH,
        )

    def all_small(n, buf):
        span = buf.at[pl.ds(0, group - 1)]
        return small(n, span, span, partner)

    @each_peer
    def _(i):
        j, to = peer(i)
        small(0, asked.at[j // per], wanted.at[me], to).start()

    @each_peer
    def _(i):
        small(1, lists.at[me], lists.at[me], peer(i)[1]).start()

    loads[1].wait()
    loads[2].wait()
    spot = place_of(sec, lo, hi)
    x = tok_ref[...].astype(F32)
    scale = lax.rsqrt(jnp.mean(x * x, axis=-1, keepdims=True) + 1e-06)
    normed = (x * scale * gain_ref[...]).astype(BF16)
    norms[spot] = normed

    def block(s, l, k):
        return place_of(s, l, turn(hi, k, nhi))

    half = tok_rows // 2
    parts = {"whole": pl.ds(0, tok_rows), "top": pl.ds(0, half), "bottom": pl.ds(half, half)}
    classes = [[0], [1], list(range(2, nhi))]
    beside = (1 - sec, view, scene)
    below = (sec, hi * nlo + 1 - lo, scene)

    def norm_copy(n, ref, to):
        return pltpu.make_async_remote_copy(
            src_ref=ref, dst_ref=ref, send_sem=s_norm.at[n], recv_sem=r_norm.at[n],
            device_id=to, device_id_type=MESH,
        )

    flows = {
        "x": (3, beside, sec, lo, "whole"),
        "y": (6, below, sec, lo, "whole"),
        "far_x": (9, beside, sec, 1 - lo, "top"),
        "far_y": (12, below, 1 - sec, lo, "bottom"),
    }

    def line_send(c):
        for k in classes[c]:
            to = (sec, turn(hi, k, nhi) * nlo + lo, scene)
            norm_copy(c, norms.at[block(sec, lo, 0)], to).start()

    def flow_send(name, c):
        n, to, s, l, part = flows[name]
        for k in classes[c]:
            norm_copy(n + c, norms.at[block(s, l, k), parts[part]], to).start()

    def flow_all(name, c):
        n, _, _, _, part = flows[name]
        return norm_copy(n + c, norms.at[pl.ds(0, len(classes[c])), parts[part]], partner)

    def line_all(c):
        return norm_copy(c, norms.at[pl.ds(0, len(classes[c]))], partner)

    line_send(1)
    flow_send("x", 0)
    flow_send("y", 0)
    line_send(2)

    loads[3].wait()
    head = mm(normed, w_ref[...], NN)
    stack = jnp.concatenate(
        [head[:, p * gpt : (p + 1) * gpt] for p in range(PARAMS)], axis=0
    ).astype(BF16)
    er = lax.broadcasted_iota(jnp.int32, (PARAMS * tok_rows, PARAMS * tok_rows), 0)
    ec = lax.broadcasted_iota(jnp.int32, (PARAMS * tok_rows, PARAMS * tok_rows), 1)
    swap = jnp.where(ec == (er % PARAMS) * tok_rows + er // PARAMS, 1.0, 0.0).astype(BF16)
    table = mm(swap, stack, NN).astype(BF16)

    lane = lax.broadcasted_iota(jnp.int32, (8, 128), 1)
    mine_at = lax.rem(me, per)

    def gathered(buf):
        out = []
        for i in range(packs):
            total = None
            for k in range(per):
                q = lax.rem(mine_at + k, per)
                block = buf[i * per + q].astype(F32)
                if k:
                    block = pltpu.roll(block, k * cap, 1)
                total = block if total is None else jnp.where(lane[: block.shape[0]] // cap == q, block, total)
            out.append(total)
        return jnp.concatenate(out, axis=1)

    all_small(0, wanted).wait_recv()
    asks_in = gathered(wanted)
    ask = asks_in.astype(jnp.int32)
    ask_t = ask // gpt
    ask_g = ask - ask_t * gpt
    hot = jnp.where(
        lax.broadcasted_iota(jnp.int32, (gpt, group * cap), 0) == ask_g, 1.0, 0.0
    ).astype(BF16)
    spread_rows = mm(table, hot, NN)
    answer = jnp.zeros((PARAMS, group * cap), F32)
    for t in range(tok_rows):
        answer = jnp.where(
            ask_t == t, spread_rows[t * PARAMS : (t + 1) * PARAMS], answer
        )
    for i in range(packs):
        found[i] = answer[:, i * 128 : (i + 1) * 128].astype(BF16)
    given[me] = found[me // per]

    @each_peer
    def _(i):
        j, to = peer(i)
        small(2, found.at[j // per], given.at[me], to).start()

    stretch = nhi * tok_rows

    def turn_line(s, l):
        n = s * nlo + l
        turned[n] = norms[pl.ds(n * nhi, nhi)].reshape(stretch, width).T

    line_all(1).wait_recv()
    flow_send("x", 1)
    flow_send("y", 1)
    flow_all("x", 0).wait_recv()
    flow_all("y", 0).wait_recv()
    flow_send("far_x", 0)
    flow_send("far_y", 0)
    all_small(1, lists).wait_recv()
    row_at = lax.broadcasted_iota(jnp.int32, (tokens, K), 0)
    gauss_at = lax.broadcasted_iota(jnp.int32, (gpt, K), 0)

    def mark_rows(g, n):
        for q in range(batch):
            j = peer(g * batch + q)[0]
            for b in range(tiles):
                at = lists[j, pl.ds(b, 1), :] // gpt
                where[n, :, (q * tiles + b) * K : (q * tiles + b + 1) * K] = jnp.where(
                    row_at == at, 1.0, 0.0
                ).astype(BF16)

    @pl.loop(0, group // batch)
    def _(g):
        if ahead:
            mark_rows(g, g)

    @pl.loop(0, group)
    def _(j):
        for b in range(tiles):
            at = lists[j, pl.ds(b, 1), :]
            at = at - (at // gpt) * gpt
            fits[j, :, b * K : (b + 1) * K] = jnp.where(gauss_at == at, 1.0, 0.0).astype(BF16)

    line_all(2).wait_recv()
    flow_send("x", 2)
    flow_send("y", 2)
    flow_all("x", 1).wait_recv()
    flow_all("y", 1).wait_recv()
    flow_send("far_x", 1)
    flow_send("far_y", 1)
    turn_line(sec, lo)
    all_small(2, given).wait_recv()
    picked = mm(gathered(given).astype(BF16), perm[...], NN)
    rows = [picked[p : p + 1] for p in range(PARAMS)]
    loads[4].wait()

    place = lax.broadcasted_iota(jnp.int32, (1, pix), 1)
    across = ((place % SIDE).astype(F32) + 0.5) * (2.0 / SIDE) - 1.0
    down = ((place // SIDE).astype(F32) + 0.5) * (2.0 / SIDE) - 1.0
    ka = lax.broadcasted_iota(jnp.int32, (K, 2 * K), 0)
    kb = lax.rem(lax.broadcasted_iota(jnp.int32, (K, 2 * K), 1), K)
    lower = jnp.where(kb < ka, 1.0, 0.0).astype(BF16)
    upper = jnp.where(kb > ka, 1.0, 0.0).astype(BF16)
    moments = jnp.concatenate(
        [jnp.ones((1, pix), F32), across, down, across * across + down * down, jnp.zeros((4, pix), F32)],
        axis=0,
    ).astype(BF16)
    vi = me * VIEWS // group
    cam = [cam_ref[vi, n] for n in range(8)]
    slot = lax.broadcasted_iota(jnp.int32, (1, K), 1)
    live = jnp.concatenate(
        [jnp.where(slot < count_ref[b], 1.0, 0.0) for b in range(tiles)], axis=1
    )
    mx, my, mz, ls, op = rows[:5]
    sx = jnp.tanh(cam[0] * mx + cam[1] * my + cam[2] * mz + cam[3])
    sy = jnp.tanh(cam[4] * mx + cam[5] * my + cam[6] * mz + cam[7])
    spread = jnp.exp(-2.0 * ls)
    sop = sigmoid(op)
    amp = 0.3 * sop * live
    shade = sigmoid(picked[5:8])
    shade8 = jnp.concatenate([shade, jnp.zeros((5, slots), F32)], axis=0)
    steep = (-0.5 * LOG2E) * jnp.minimum(spread, 1e38)
    cols = jnp.concatenate([sx, sy, steep, amp, jnp.zeros((4, slots), F32)], axis=0).T
    cuts = [slice(b * K, (b + 1) * K) for b in range(tiles)]

    alphas, inverses, logs = [], [], []
    for cut in cuts:
        csx, csy, csp, camp = [cols[cut, n : n + 1] for n in range(4)]
        dx = across - csx
        dy = down - csy
        alpha = camp * jnp.exp2((dx * dx + dy * dy) * csp)
        rest = 1.0 - alpha
        alphas.append(alpha)
        inverses.append(alpha / rest)
        logs.append(jnp.concatenate(split(jnp.log(rest)), axis=0))
    befores = [mm(lower, x, NN) for x in logs]
    weights = [alpha * jnp.exp(before) for alpha, before in zip(alphas, befores)]
    packed = [weight.astype(BF16) for weight in weights]
    shade_hi, shade_lo = split(shade8)
    shade_two = jnp.concatenate([shade_hi, shade_lo], axis=0)
    colours = []
    for cut, weight in zip(cuts, packed):
        both = mm(shade_two[:, cut], weight, NN)
        colours.append(both[:8] + both[8:])
    loss_part = jnp.zeros((1, K), F32)
    dcols = []
    for b in range(tiles):
        want = jnp.concatenate(
            [want_ref[pl.ds(b, 1), c * pix : (c + 1) * pix].astype(F32) for c in range(3)]
            + [jnp.zeros((5, pix), F32)],
            axis=0,
        )
        for c in range(3):
            image_ref[pl.ds(b, 1), c * pix : (c + 1) * pix] = colours[b][c : c + 1].astype(BF16)
        diff = colours[b] - want
        sq = jnp.sum(diff * diff, axis=0, keepdims=True)
        for n in range(0, pix, K):
            loss_part = loss_part + sq[:, n : n + K]
        dcols.append(((2.0 * factor) * diff).astype(BF16))
    losses[me] = loss_part * factor
    dshade = jnp.concatenate([mm(d, w, NT) for d, w in zip(dcols, packed)], axis=1)
    dwws = [
        mm(shade_hi[:, cut], d, TN) * weight for cut, d, weight in zip(cuts, dcols, weights)
    ]
    dlogs = [mm(upper[:, :K], x.astype(BF16), NN) for x in dwws]
    sums = []
    for x, y, inverse in zip(dwws, dlogs, inverses):
        h = x - y * inverse
        both = mm(moments, jnp.concatenate(split(h), axis=0), NT)
        sums.append(both[:, :K] + both[:, K:])
    sums = jnp.concatenate(sums, axis=1)
    s_h, s_u, s_v, s_q = [sums[n : n + 1] for n in range(4)]
    s_x = s_u - sx * s_h
    s_y = s_v - sy * s_h
    s_r = s_q - 2.0 * (sx * s_u + sy * s_v) + (sx * sx + sy * sy) * s_h
    px = spread * s_x * (1.0 - sx * sx)
    py = spread * s_y * (1.0 - sy * sy)
    out = jnp.concatenate(
        [
            cam[0] * px + cam[4] * py,
            cam[1] * px + cam[5] * py,
            cam[2] * px + cam[6] * py,
            spread * s_r,
            (1.0 - sop) * s_h,
            dshade[0:3] * shade * (1.0 - shade),
        ],
        axis=0,
    )
    wide = slots // 2
    grads[me] = jnp.concatenate([out[:, :wide], out[:, wide:]], axis=0).astype(BF16)

    def push(n, buf, i, recv):
        j, to = peer(i)
        return pltpu.make_async_remote_copy(
            src_ref=buf.at[me], dst_ref=buf.at[me], send_sem=s_grad.at[n],
            recv_sem=recv, device_id=to, device_id_type=MESH,
        )

    @each_peer
    def _(i):
        push(0, grads, i, r_grad.at[me]).start()

    flow_all("x", 2).wait_recv()
    flow_all("y", 2).wait_recv()
    turn_line(1 - sec, lo)
    turn_line(sec, 1 - lo)

    def late_sends():
        flow_send("far_x", 2)
        flow_send("far_y", 2)

        @each_peer
        def _(i):
            push(1, losses, i, s_loss.at[1]).start()

    def gather_batch(g, n):
        sides = []
        for q in range(batch):
            i = g * batch + q
            j = peer(i)[0]
            if isinstance(i, int):
                if i > 0:
                    push(0, grads, i, r_grad.at[j]).wait_recv()
            else:
                pl.when(i > 0)(lambda: push(0, grads, i, r_grad.at[j]).wait_recv())
            got = grads[j]
            fit = fits[j]
            sides.append(
                jnp.concatenate(
                    [
                        jnp.concatenate(
                            [
                                fit[:, :wide] * got[p : p + 1],
                                fit[:, wide:] * got[PARAMS + p : PARAMS + p + 1],
                            ],
                            axis=1,
                        )
                        for p in range(PARAMS)
                    ],
                    axis=0,
                )
            )
        return mm(jnp.concatenate(sides, axis=1), where[n], NT)

    if ahead:
        dhead[...] = gather_batch(0, 0)
        for g in range(1, group // batch):
            if g == LATE:
                late_sends()
            dhead[...] += gather_batch(g, g)
    else:
        late_sends()
        dhead[...] = jnp.zeros_like(dhead)

        @pl.loop(0, group // batch)
        def _(g):
            mark_rows(g, 0)
            dhead[...] += gather_batch(g, 0)

    loss_all = losses.at[pl.ds(0, group - 1)]
    pltpu.make_async_remote_copy(
        src_ref=loss_all, dst_ref=loss_all, send_sem=s_grad.at[1], recv_sem=s_loss.at[1],
        device_id=partner, device_id_type=MESH,
    ).wait_recv()
    loss_mine[...] = jnp.broadcast_to(jnp.sum(losses[...], axis=0), loss_mine.shape)
    for name in ("far_x", "far_y"):
        for c in range(3):
            flow_all(name, c).wait_recv()
    turn_line(1 - sec, 1 - lo)
    loss_copy = pltpu.make_async_remote_copy(
        src_ref=loss_mine, dst_ref=loss_theirs, send_sem=s_loss.at[0], recv_sem=r_loss,
        device_id=partner, device_id_type=MESH,
    )
    dh = dhead[...].astype(BF16)
    dhead_rows = 256
    chunks = width // dhead_rows

    def part_copy(n):
        span = pl.ds(n * dhead_rows, dhead_rows)
        return pltpu.make_async_remote_copy(
            src_ref=mine.at[span], dst_ref=theirs.at[span],
            send_sem=s_part.at[n], recv_sem=r_part.at[n],
            device_id=partner, device_id_type=MESH,
        )

    for n in range(chunks):
        span = slice(n * dhead_rows, (n + 1) * dhead_rows)
        side = jnp.concatenate([turned[m, span] for m in range(nsec * nlo)], axis=1)
        mine[span, :] = mm(side, dh, NT).astype(BF16)
        if n == 0:
            loss_copy.start()
        else:
            part_copy(n - 1).start()
    part_copy(chunks - 1).start()

    for n in range(chunks):
        part_copy(n).wait_recv()
        span = slice(n * dhead_rows, (n + 1) * dhead_rows)
        grad_ref[span, :] = mine[span, :].astype(F32) + theirs[span, :].astype(F32)
    loss_copy.wait_recv()
    loss_ref[...] = jnp.sum(loss_mine[0:1] + loss_theirs[0:1], keepdims=True)

    loss_copy.wait_send()
    for n in range(chunks):
        part_copy(n).wait_send()
    all_small(0, wanted).wait_send()
    all_small(1, lists).wait_send()
    all_small(2, given).wait_send()
    grad_all = grads.at[pl.ds(0, group - 1)]
    pltpu.make_async_remote_copy(
        src_ref=grad_all, dst_ref=grad_all, send_sem=s_grad.at[0], recv_sem=r_grad.at[0],
        device_id=partner, device_id_type=MESH,
    ).wait_send()
    pltpu.make_async_remote_copy(
        src_ref=loss_all, dst_ref=loss_all, send_sem=s_grad.at[1], recv_sem=s_loss.at[1],
        device_id=partner, device_id_type=MESH,
    ).wait_send()
    line_all(1).wait_send()
    line_all(2).wait_send()
    for name in flows:
        for c in range(3):
            flow_all(name, c).wait_send()


def store(image_ref, grad_ref, loss_ref, image_out, grad_out, loss_out, sems):
    pairs = [(image_ref, image_out), (loss_ref, loss_out)]
    rows = grad_ref.shape[0] // STORES
    for n in range(STORES):
        span = pl.ds(n * rows, rows)
        pairs.append((grad_ref.at[span], grad_out.at[span]))
    copies = [pltpu.make_async_copy(src, dst, sems.at[n]) for n, (src, dst) in enumerate(pairs)]
    for copy in copies:
        copy.start()
    for copy in copies:
        copy.wait()


def solution(mesh):
    nsec, nview, nscene = mesh.shape["section"], mesh.shape["view"], mesh.shape["scene"]
    group = nsec * nview
    nlo = 2
    assert nsec == 2 and nview % 8 == 0

    def body(tokens, norm_gain, head_weight, tile_lists, tile_counts, cameras, targets):
        tok_rows, width = tokens.shape[1:]
        outw = head_weight.shape[1]
        gpt = outw // PARAMS
        tiles, K = tile_lists.shape[1:]
        slots = tiles * K
        cap = 2 * slots // group
        packs = group * cap // 128
        factor = 1.0 / (nscene * tiles * group)
        ahead = group * group * tok_rows * slots <= 2**24
        batch = min(BATCH, group)
        vmem = pl.BlockSpec(memory_space=pltpu.VMEM)
        smem = pl.BlockSpec(memory_space=pltpu.SMEM)
        hbm = pl.BlockSpec(memory_space=pltpu.HBM)
        dma = pltpu.SemaphoreType.DMA
        image, grad, loss = pl.pallas_call(
            functools.partial(kernel, nsec, nview, factor),
            out_shape=(
                pltpu.VMEM((tiles, targets.shape[2]), BF16),
                pltpu.VMEM((width, outw), F32),
                pltpu.VMEM((1, 1), F32),
            ),
            in_specs=[hbm, hbm, hbm, hbm, smem, smem, hbm],
            out_specs=(vmem, vmem, vmem),
            scratch_shapes=[
                pltpu.VMEM((tok_rows, width), BF16),
                pltpu.VMEM((1, width), F32),
                pltpu.VMEM((width, outw), BF16),
                pltpu.VMEM((tiles, K), jnp.int32),
                pltpu.VMEM((tiles, targets.shape[2]), BF16),
                pltpu.VMEM((group * cap, slots), BF16),
                pltpu.VMEM((packs, 1, 128), F32),
                pltpu.VMEM((group, 1, 128), F32),
                pltpu.VMEM((packs, PARAMS, 128), BF16),
                pltpu.VMEM((group, PARAMS, 128), BF16),
                pltpu.VMEM((group, tiles, K), jnp.int32),
                pltpu.VMEM((group // batch if ahead else 1, group * tok_rows, batch * slots), BF16),
                pltpu.VMEM((group, gpt, slots), BF16),
                pltpu.VMEM((group, tok_rows, width), BF16),
                pltpu.VMEM((group, 2 * PARAMS, slots // 2), BF16),
                pltpu.VMEM((outw, group * tok_rows), F32),
                pltpu.VMEM((nsec * nlo, width, group * tok_rows // (nsec * nlo)), BF16),
                pltpu.VMEM((width, outw), BF16),
                pltpu.VMEM((width, outw), BF16),
                pltpu.VMEM((group, 1, K), F32),
                pltpu.VMEM((8, K), F32),
                pltpu.VMEM((8, K), F32),
                dma((5,)),
                dma((3,)), dma((3,)),
                dma((15,)), dma((15,)),
                dma((2,)), dma((group,)),
                dma((width // 256,)), dma((width // 256,)),
                dma((2,)), dma,
            ],
            compiler_params=pltpu.CompilerParams(
                collective_id=0, has_side_effects=True, vmem_limit_bytes=61 * 1024 * 1024
            ),
        )(
            tokens[0], norm_gain[None], head_weight, tile_lists[0], tile_counts[0], cameras[0],
            targets[0],
        )
        image, grad, loss = pl.pallas_call(
            store,
            out_shape=tuple(
                jax.ShapeDtypeStruct(x.shape, x.dtype) for x in (image, grad, loss)
            ),
            in_specs=[vmem] * 3,
            out_specs=(hbm,) * 3,
            scratch_shapes=[dma((2 + STORES,))],
            compiler_params=pltpu.CompilerParams(vmem_limit_bytes=1024 * 1024),
        )(image, grad, loss)
        return image[None], grad, loss[0, 0]

    in_specs = (
        P("scene", ("section", "view"), None),
        P(),
        P(),
        P("scene", ("section", "view"), None),
        P("scene", ("section", "view")),
        P("scene", None, None),
        P("scene", ("section", "view"), None),
    )
    out_specs = (P("scene", ("section", "view"), None), P(), P())
    return jax.shard_map(body, mesh=mesh, in_specs=in_specs, out_specs=out_specs, check_vma=False)
```

```python
import functools

import jax
import jax.numpy as jnp
from jax import lax
from jax.experimental import pallas as pl
from jax.experimental.pallas import tpu as pltpu
from jax.sharding import PartitionSpec as P

PARAMS = 8
ROWS = 7
SIDE = 16
BATCH = 2
FINISH = 0
LATE = 1
VIEWS = 2
MESH = pl.DeviceIdType.MESH
F32 = jnp.float32
BF16 = jnp.bfloat16
LOG2E = 1.4426950408889634
NN = (((1,), (0,)), ((), ()))
NT = (((1,), (1,)), ((), ()))
TN = (((0,), (0,)), ((), ()))


def mm(a, b, dims):
    return lax.dot_general(a, b, dims, preferred_element_type=F32)


def split(x):
    hi = x.astype(BF16)
    lo = (x - hi.astype(F32)).astype(BF16)
    return hi, lo


def sigmoid(x):
    return 1.0 / (1.0 + jnp.exp(-x))


def turn(a, k, n):
    if n & (n - 1):
        return lax.rem(a + k, n)
    if isinstance(k, int):
        bit = 1
        while bit < n:
            if k & bit:
                a = a + bit - 2 * bit * lax.rem(a // bit, 2)
            bit *= 2
        return a
    out, bit = 0, 1
    while bit < n:
        out = out + bit * lax.rem((a // bit) + (k // bit), 2)
        bit *= 2
    return out


def kernel(
    nsec, nview, factor,
    tok_hbm, gain_hbm, w_hbm, list_hbm, count_ref, cam_ref, want_hbm,
    image_ref, grad_ref, loss_ref,
    tok_ref, gain_ref, w_ref, list_ref, want_ref,
    perm, asked, wanted, found, given, lists, where, fits, norms, grads, dhead, turned, turned_far, mine, theirs,
    losses, loss_mine, loss_theirs,
    s_in, s_small, r_small, s_norm, r_norm, s_grad, r_grad, s_part, r_part, s_loss, r_loss, s_turn, r_turn,
):
    group = nsec * nview
    nlo = 2
    nhi = nview // nlo
    sec, view, scene = lax.axis_index("section"), lax.axis_index("view"), lax.axis_index("scene")
    hi, lo = view // nlo, lax.rem(view, nlo)
    me = sec * nview + view
    tok_rows, width = tok_ref.shape
    outw = w_ref.shape[1]
    gpt = outw // PARAMS
    tiles, K = list_ref.shape
    slots = tiles * K
    tokens = group * tok_rows
    pix = SIDE * SIDE
    cap = 2 * slots // group
    per = 128 // cap
    packs = group // per
    ahead = where.shape[0] > 1
    batch = where.shape[2] // slots

    def local(n, src, dst):
        return pltpu.make_async_copy(src, dst, s_in.at[n])

    loads = [
        local(0, list_hbm, list_ref),
        local(1, tok_hbm, tok_ref),
        local(2, gain_hbm, gain_ref),
        local(3, w_hbm, w_ref),
        local(4, want_hbm, want_ref),
    ]
    for load in loads:
        load.start()

    known = {}

    def each_peer(act):
        if group <= 16:
            for i in range(group - 1, 0, -1):
                act(i)
        else:
            pl.loop(1, group)(act)

    def peer(i):
        if isinstance(i, int):
            if i not in known:
                known[i] = find(i)
            return known[i]
        return find(i)

    def find(i):
        s = turn(sec, i % nsec, nsec)
        l = turn(lo, (i // nsec) % nlo, nlo)
        h = turn(hi, i // (nsec * nlo), nhi)
        v = h * nlo + l
        return s * nview + v, (s, v, scene)

    def place_of(s, l, h):
        return (s * nlo + l) * nhi + h

    partner = (sec, view, 1 - scene)
    barrier = pltpu.get_barrier_semaphore()

    @each_peer
    def _(i):
        pl.semaphore_signal(barrier, inc=1, device_id=peer(i)[1], device_id_type=MESH)

    pl.semaphore_signal(barrier, inc=1, device_id=partner, device_id_type=MESH)

    loads[0].wait()
    number = jnp.concatenate([list_ref[pl.ds(b, 1), :] for b in range(tiles)], axis=1)
    token = number // gpt
    gauss = number - token * gpt
    owner = token // tok_rows
    inner = token - owner * tok_rows
    ow_sec = owner // nview
    ow_hi = (owner - ow_sec * nview) // nlo
    ow_lo = owner - ow_sec * nview - ow_hi * nlo
    row = place_of(ow_sec, ow_lo, ow_hi) * tok_rows + inner
    code = row * gpt + gauss
    for b in range(tiles):
        lists[me, pl.ds(b, 1), :] = code[:, b * K : (b + 1) * K]
    mask = jnp.where(lax.broadcasted_iota(jnp.int32, (group, slots), 0) == owner, 1.0, 0.0)
    earlier = jnp.where(
        lax.broadcasted_iota(jnp.int32, (slots, slots), 0)
        < lax.broadcasted_iota(jnp.int32, (slots, slots), 1),
        1.0, 0.0,
    ).astype(BF16)
    rank = jnp.sum(mask * mm(mask.astype(BF16), earlier, NN), axis=0, keepdims=True)
    dest = owner * cap + rank.astype(jnp.int32)
    perm[...] = jnp.where(
        lax.broadcasted_iota(jnp.int32, (group * cap, slots), 0) == dest, 1.0, 0.0
    ).astype(BF16)
    asks = jnp.concatenate(
        [inner.astype(F32), gauss.astype(F32), jnp.zeros((6, slots), F32)], axis=0
    ).astype(BF16)
    requests = mm(asks, perm[...], NT)
    requests = requests[0:1] * float(gpt) + requests[1:2]
    for i in range(packs):
        asked[i] = requests[:, i * 128 : (i + 1) * 128]
    wanted[me] = asked[me // per]

    pl.semaphore_wait(barrier, group)

    def small(n, src, dst, where_to):
        return pltpu.make_async_remote_copy(
            src_ref=src, dst_ref=dst, send_sem=s_small.at[n], recv_sem=r_small.at[n],
            device_id=where_to, device_id_type=MESH,
        )

    def all_small(n, buf):
        span = buf.at[pl.ds(0, group - 1)]
        return small(n, span, span, partner)

    @each_peer
    def _(i):
        j, to = peer(i)
        small(0, asked.at[j // per], wanted.at[me], to).start()

    @each_peer
    def _(i):
        small(1, lists.at[me], lists.at[me], peer(i)[1]).start()

    loads[1].wait()
    loads[2].wait()
    spot = place_of(sec, lo, hi)
    x = tok_ref[...].astype(F32)
    scale = lax.rsqrt(jnp.mean(x * x, axis=-1, keepdims=True) + 1e-06)
    normed = (x * scale * gain_ref[...]).astype(BF16)
    norms[spot] = normed

    def block(s, l, k):
        return place_of(s, l, turn(hi, k, nhi))

    half = tok_rows // 2
    parts = {"whole": pl.ds(0, tok_rows), "top": pl.ds(0, half), "bottom": pl.ds(half, half)}
    classes = [[0], [1], list(range(2, nhi))]
    beside = (1 - sec, view, scene)
    below = (sec, hi * nlo + 1 - lo, scene)

    def norm_copy(n, ref, to):
        return pltpu.make_async_remote_copy(
            src_ref=ref, dst_ref=ref, send_sem=s_norm.at[n], recv_sem=r_norm.at[n],
            device_id=to, device_id_type=MESH,
        )

    flows = {
        "x": (3, beside, sec, lo, "whole"),
        "y": (6, below, sec, lo, "whole"),
        "far_x": (9, beside, sec, 1 - lo, "top"),
        "far_y": (12, below, 1 - sec, lo, "bottom"),
    }

    def line_send(c):
        for k in classes[c]:
            to = (sec, turn(hi, k, nhi) * nlo + lo, scene)
            norm_copy(c, norms.at[block(sec, lo, 0)], to).start()

    def flow_send(name, c):
        n, to, s, l, part = flows[name]
        for k in classes[c]:
            norm_copy(n + c, norms.at[block(s, l, k), parts[part]], to).start()

    def flow_all(name, c):
        n, _, _, _, part = flows[name]
        return norm_copy(n + c, norms.at[pl.ds(0, len(classes[c])), parts[part]], partner)

    def line_all(c):
        return norm_copy(c, norms.at[pl.ds(0, len(classes[c]))], partner)

    line_send(1)
    flow_send("x", 0)
    flow_send("y", 0)
    line_send(2)

    loads[3].wait()
    head = mm(normed, w_ref[...], NN)
    stack = jnp.concatenate(
        [head[:, p * gpt : (p + 1) * gpt] for p in range(PARAMS)], axis=0
    ).astype(BF16)
    er = lax.broadcasted_iota(jnp.int32, (PARAMS * tok_rows, PARAMS * tok_rows), 0)
    ec = lax.broadcasted_iota(jnp.int32, (PARAMS * tok_rows, PARAMS * tok_rows), 1)
    swap = jnp.where(ec == (er % PARAMS) * tok_rows + er // PARAMS, 1.0, 0.0).astype(BF16)
    table = mm(swap, stack, NN).astype(BF16)

    lane = lax.broadcasted_iota(jnp.int32, (8, 128), 1)
    mine_at = lax.rem(me, per)

    def gathered(buf):
        out = []
        for i in range(packs):
            total = None
            for k in range(per):
                q = lax.rem(mine_at + k, per)
                block = buf[i * per + q].astype(F32)
                if k:
                    block = pltpu.roll(block, k * cap, 1)
                total = block if total is None else jnp.where(lane[: block.shape[0]] // cap == q, block, total)
            out.append(total)
        return jnp.concatenate(out, axis=1)

    all_small(0, wanted).wait_recv()
    asks_in = gathered(wanted)
    ask = asks_in.astype(jnp.int32)
    ask_t = ask // gpt
    ask_g = ask - ask_t * gpt
    hot = jnp.where(
        lax.broadcasted_iota(jnp.int32, (gpt, group * cap), 0) == ask_g, 1.0, 0.0
    ).astype(BF16)
    spread_rows = mm(table, hot, NN)
    answer = jnp.zeros((PARAMS, group * cap), F32)
    for t in range(tok_rows):
        answer = jnp.where(
            ask_t == t, spread_rows[t * PARAMS : (t + 1) * PARAMS], answer
        )
    for i in range(packs):
        found[i] = answer[:, i * 128 : (i + 1) * 128].astype(BF16)
    given[me] = found[me // per]

    @each_peer
    def _(i):
        j, to = peer(i)
        small(2, found.at[j // per], given.at[me], to).start()

    stretch = nhi * tok_rows

    def turn_copy(m, s, l):
        n = s * nlo + l
        return pltpu.make_async_remote_copy(
            src_ref=turned.at[n], dst_ref=turned_far.at[n], send_sem=s_turn.at[m],
            recv_sem=r_turn.at[m], device_id=partner, device_id_type=MESH,
        )

    def turn_line(m, s, l):
        n = s * nlo + l
        turned[n] = norms[pl.ds(n * nhi, nhi)].reshape(stretch, width).T
        turn_copy(m, s, l).start()

    line_all(1).wait_recv()
    flow_send("x", 1)
    flow_send("y", 1)
    flow_all("x", 0).wait_recv()
    flow_all("y", 0).wait_recv()
    flow_send("far_x", 0)
    flow_send("far_y", 0)
    all_small(1, lists).wait_recv()
    row_at = lax.broadcasted_iota(jnp.int32, (tokens, K), 0)
    gauss_at = lax.broadcasted_iota(jnp.int32, (gpt, K), 0)

    def source(g, q):
        return (g // 2) * (2 * batch) + g % 2 + 2 * q

    def mark_rows(g, n):
        for q in range(batch):
            j = peer(source(g, q))[0]
            for b in range(tiles):
                at = lists[j, pl.ds(b, 1), :] // gpt
                where[n, :, (q * tiles + b) * K : (q * tiles + b + 1) * K] = jnp.where(
                    row_at == at, 1.0, 0.0
                ).astype(BF16)

    @pl.loop(0, group // batch)
    def _(g):
        if ahead:
            mark_rows(g, g)

    @pl.loop(0, group)
    def _(j):
        for b in range(tiles):
            at = lists[j, pl.ds(b, 1), :]
            at = at - (at // gpt) * gpt
            fits[j, :, b * K : (b + 1) * K] = jnp.where(gauss_at == at, 1.0, 0.0).astype(BF16)

    line_all(2).wait_recv()
    flow_send("x", 2)
    flow_send("y", 2)
    flow_all("x", 1).wait_recv()
    flow_all("y", 1).wait_recv()
    flow_send("far_x", 1)
    flow_send("far_y", 1)
    turn_line(0, sec, lo)
    all_small(2, given).wait_recv()
    picked = mm(gathered(given).astype(BF16), perm[...], NN)
    rows = [picked[p : p + 1] for p in range(PARAMS)]
    loads[4].wait()

    place = lax.broadcasted_iota(jnp.int32, (1, pix), 1)
    across = ((place % SIDE).astype(F32) + 0.5) * (2.0 / SIDE) - 1.0
    down = ((place // SIDE).astype(F32) + 0.5) * (2.0 / SIDE) - 1.0
    ka = lax.broadcasted_iota(jnp.int32, (K, 2 * K), 0)
    kb = lax.rem(lax.broadcasted_iota(jnp.int32, (K, 2 * K), 1), K)
    lower = jnp.where(kb < ka, 1.0, 0.0).astype(BF16)
    upper = jnp.where(kb > ka, 1.0, 0.0).astype(BF16)
    moments = jnp.concatenate(
        [jnp.ones((1, pix), F32), across, down, across * across + down * down, jnp.zeros((4, pix), F32)],
        axis=0,
    ).astype(BF16)
    cam = [cam_ref[sec, n] for n in range(8)]
    cam_far = [cam_ref[1 - sec, n] for n in range(8)]
    slot = lax.broadcasted_iota(jnp.int32, (1, K), 1)
    live = jnp.concatenate(
        [jnp.where(slot < count_ref[b], 1.0, 0.0) for b in range(tiles)], axis=1
    )
    mx, my, mz, ls, op = rows[:5]
    sx = jnp.tanh(cam[0] * mx + cam[1] * my + cam[2] * mz + cam[3])
    sy = jnp.tanh(cam[4] * mx + cam[5] * my + cam[6] * mz + cam[7])
    spread = jnp.exp(-2.0 * ls)
    sop = sigmoid(op)
    amp = 0.3 * sop * live
    shade = sigmoid(picked[5:8])
    shade8 = jnp.concatenate([shade, jnp.zeros((5, slots), F32)], axis=0)
    steep = (-0.5 * LOG2E) * jnp.minimum(spread, 1e38)
    cols = jnp.concatenate([sx, sy, steep, amp, jnp.zeros((4, slots), F32)], axis=0).T
    cuts = [slice(b * K, (b + 1) * K) for b in range(tiles)]

    alphas, inverses, logs = [], [], []
    for cut in cuts:
        csx, csy, csp, camp = [cols[cut, n : n + 1] for n in range(4)]
        dx = across - csx
        dy = down - csy
        alpha = camp * jnp.exp2((dx * dx + dy * dy) * csp)
        rest = 1.0 - alpha
        alphas.append(alpha)
        inverses.append(alpha / rest)
        logs.append(jnp.concatenate(split(jnp.log(rest)), axis=0))
    befores = [mm(lower, x, NN) for x in logs]
    weights = [alpha * jnp.exp(before) for alpha, before in zip(alphas, befores)]
    packed = [weight.astype(BF16) for weight in weights]
    shade_hi, shade_lo = split(shade8)
    shade_two = jnp.concatenate([shade_hi, shade_lo], axis=0)
    colours = []
    for cut, weight in zip(cuts, packed):
        both = mm(shade_two[:, cut], weight, NN)
        colours.append(both[:8] + both[8:])
    loss_part = jnp.zeros((1, K), F32)
    dcols = []
    for b in range(tiles):
        want = jnp.concatenate(
            [want_ref[pl.ds(b, 1), c * pix : (c + 1) * pix].astype(F32) for c in range(3)]
            + [jnp.zeros((5, pix), F32)],
            axis=0,
        )
        for c in range(3):
            image_ref[pl.ds(b, 1), c * pix : (c + 1) * pix] = colours[b][c : c + 1].astype(BF16)
        diff = colours[b] - want
        sq = jnp.sum(diff * diff, axis=0, keepdims=True)
        for n in range(0, pix, K):
            loss_part = loss_part + sq[:, n : n + K]
        dcols.append(((2.0 * factor) * diff).astype(BF16))
    losses[me] = loss_part * factor
    dshade = jnp.concatenate([mm(d, w, NT) for d, w in zip(dcols, packed)], axis=1)
    dwws = [
        mm(shade_hi[:, cut], d, TN) * weight for cut, d, weight in zip(cuts, dcols, weights)
    ]
    dlogs = [mm(upper[:, :K], x.astype(BF16), NN) for x in dwws]
    sums = []
    for x, y, inverse in zip(dwws, dlogs, inverses):
        h = x - y * inverse
        both = mm(moments, jnp.concatenate(split(h), axis=0), NT)
        sums.append(both[:, :K] + both[:, K:])
    sums = jnp.concatenate(sums, axis=1)
    s_h, s_u, s_v, s_q = [sums[n : n + 1] for n in range(4)]
    s_x = s_u - sx * s_h
    s_y = s_v - sy * s_h
    s_r = s_q - 2.0 * (sx * s_u + sy * s_v) + (sx * sx + sy * sy) * s_h
    px = spread * s_x * (1.0 - sx * sx)
    py = spread * s_y * (1.0 - sy * sy)
    out = jnp.concatenate(
        [
            px,
            py,
            spread * s_r,
            (1.0 - sop) * s_h,
            dshade[0:3] * shade * (1.0 - shade),
            jnp.zeros((1, slots), F32),
        ],
        axis=0,
    )
    wide = slots // 2
    grads[me] = jnp.concatenate([out[:, :wide], out[:, wide:]], axis=0).astype(BF16)

    def push(n, buf, i, recv):
        j, to = peer(i)
        return pltpu.make_async_remote_copy(
            src_ref=buf.at[me], dst_ref=buf.at[me], send_sem=s_grad.at[n],
            recv_sem=recv, device_id=to, device_id_type=MESH,
        )

    @each_peer
    def _(i):
        push(0, grads, i, r_grad.at[me]).start()

    flow_all("x", 2).wait_recv()
    flow_all("y", 2).wait_recv()
    turn_line(1, 1 - sec, lo)
    turn_line(2, sec, 1 - lo)

    def late_sends():
        flow_send("far_x", 2)
        flow_send("far_y", 2)

        @each_peer
        def _(i):
            push(1, losses, i, s_loss.at[1]).start()

    def gather_batch(g, n):
        sides = []
        for q in range(batch):
            i = source(g, q)
            j = peer(i)[0]
            if isinstance(i, int):
                if i > 0:
                    push(0, grads, i, r_grad.at[j]).wait_recv()
            else:
                pl.when(i > 0)(lambda: push(0, grads, i, r_grad.at[j]).wait_recv())
            got = grads[j]
            fit = fits[j]
            sides.append(
                jnp.concatenate(
                    [
                        jnp.concatenate(
                            [
                                fit[:, :wide] * got[p : p + 1],
                                fit[:, wide:] * got[PARAMS + p : PARAMS + p + 1],
                            ],
                            axis=1,
                        )
                        for p in range(ROWS)
                    ],
                    axis=0,
                )
            )
        return mm(jnp.concatenate(sides, axis=1), where[n], NT)

    def finish_turning():
        for name in ("far_x", "far_y"):
            for c in range(3):
                flow_all(name, c).wait_recv()
        turn_line(3, 1 - sec, 1 - lo)

    last = group // batch - 1
    if ahead:
        for g in range(last + 1):
            if g == LATE:
                late_sends()
            if g == last + FINISH:
                finish_turning()
            if g < 2:
                dhead[g] = gather_batch(g, g)
            else:
                dhead[g % 2] += gather_batch(g, g)
        if FINISH > 0:
            finish_turning()
    else:
        late_sends()
        dhead[...] = jnp.zeros_like(dhead)

        @pl.loop(0, last + 1)
        def _(g):
            mark_rows(g, 0)
            dhead[g % 2] += gather_batch(g, 0)

        finish_turning()

    loss_all = losses.at[pl.ds(0, group - 1)]
    pltpu.make_async_remote_copy(
        src_ref=loss_all, dst_ref=loss_all, send_sem=s_grad.at[1], recv_sem=s_loss.at[1],
        device_id=partner, device_id_type=MESH,
    ).wait_recv()
    loss_mine[...] = jnp.broadcast_to(jnp.sum(losses[...], axis=0), loss_mine.shape)
    loss_copy = pltpu.make_async_remote_copy(
        src_ref=loss_mine, dst_ref=loss_theirs, send_sem=s_loss.at[0], recv_sem=r_loss,
        device_id=partner, device_id_type=MESH,
    )
    chunk = outw // 2
    dhead_rows = 256
    chunks = width // dhead_rows

    def part_copy(c):
        span = pl.ds(c * chunk, chunk)
        return pltpu.make_async_remote_copy(
            src_ref=mine.at[span], dst_ref=theirs.at[span],
            send_sem=s_part.at[c], recv_sem=r_part.at[c],
            device_id=partner, device_id_type=MESH,
        )

    def share(v, n):
        return dhead[v, n * gpt : (n + 1) * gpt]

    for p in range(PARAMS):
        if p < 3:
            value = (
                cam[p] * share(0, 0) + cam[p + 4] * share(0, 1)
                + cam_far[p] * share(1, 0) + cam_far[p + 4] * share(1, 1)
            )
        else:
            value = share(0, p - 1) + share(1, p - 1)
        mine[p * gpt : (p + 1) * gpt] = value.astype(BF16)
        if (p + 1) * gpt % chunk == 0:
            part_copy((p + 1) * gpt // chunk - 1).start()
    loss_copy.start()

    def sides(buf, n):
        span = slice(n * dhead_rows, (n + 1) * dhead_rows)
        return span, jnp.concatenate([buf[m, span] for m in range(nsec * nlo)], axis=1)

    dh = mine[...]
    for n in range(chunks):
        span, side = sides(turned, n)
        grad_ref[span, :] = mm(side, dh, NT)
    for m in range(nsec * nlo):
        turn_copy(m, 0, 0).wait_recv()
    for c in range(2):
        part_copy(c).wait_recv()
        cut = slice(c * chunk, (c + 1) * chunk)
        dh = theirs[cut]
        for n in range(chunks):
            span, side = sides(turned_far, n)
            grad_ref[span, cut] += mm(side, dh, NT)
    loss_copy.wait_recv()
    loss_ref[...] = jnp.broadcast_to(
        jnp.sum(loss_mine[0:1] + loss_theirs[0:1], keepdims=True), loss_ref.shape
    )

    loss_copy.wait_send()
    for c in range(2):
        part_copy(c).wait_send()
    for m in range(nsec * nlo):
        turn_copy(m, 0, 0).wait_send()
    all_small(0, wanted).wait_send()
    all_small(1, lists).wait_send()
    all_small(2, given).wait_send()
    grad_all = grads.at[pl.ds(0, group - 1)]
    pltpu.make_async_remote_copy(
        src_ref=grad_all, dst_ref=grad_all, send_sem=s_grad.at[0], recv_sem=r_grad.at[0],
        device_id=partner, device_id_type=MESH,
    ).wait_send()
    pltpu.make_async_remote_copy(
        src_ref=loss_all, dst_ref=loss_all, send_sem=s_grad.at[1], recv_sem=s_loss.at[1],
        device_id=partner, device_id_type=MESH,
    ).wait_send()
    line_all(1).wait_send()
    line_all(2).wait_send()
    for name in flows:
        for c in range(3):
            flow_all(name, c).wait_send()


def store(image_ref, grad_ref, loss_ref, image_out, grad_out, loss_out, one, sems):
    pairs = [(grad_ref, grad_out), (image_ref, image_out), (one, loss_out)]
    copies = [pltpu.make_async_copy(src, dst, sems.at[n]) for n, (src, dst) in enumerate(pairs)]
    one[...] = loss_ref[0:1, 0:1]
    for copy in copies:
        copy.start()
    for copy in copies:
        copy.wait()


def solution(mesh):
    nsec, nview, nscene = mesh.shape["section"], mesh.shape["view"], mesh.shape["scene"]
    group = nsec * nview
    nlo = 2
    assert nsec == 2 and nview % 8 == 0

    def body(tokens, norm_gain, head_weight, tile_lists, tile_counts, cameras, targets):
        tok_rows, width = tokens.shape[1:]
        outw = head_weight.shape[1]
        gpt = outw // PARAMS
        tiles, K = tile_lists.shape[1:]
        slots = tiles * K
        cap = 2 * slots // group
        packs = group * cap // 128
        factor = 1.0 / (nscene * tiles * group)
        ahead = group * group * tok_rows * slots <= 2**24
        batch = min(BATCH, group)
        vmem = pl.BlockSpec(memory_space=pltpu.VMEM)
        smem = pl.BlockSpec(memory_space=pltpu.SMEM)
        hbm = pl.BlockSpec(memory_space=pltpu.HBM)
        dma = pltpu.SemaphoreType.DMA
        image, grad, loss = pl.pallas_call(
            functools.partial(kernel, nsec, nview, factor),
            out_shape=(
                pltpu.VMEM((tiles, targets.shape[2]), BF16),
                pltpu.VMEM((width, outw), F32),
                pltpu.VMEM((8, 128), F32),
            ),
            in_specs=[hbm, hbm, hbm, hbm, smem, smem, hbm],
            out_specs=(vmem, vmem, vmem),
            scratch_shapes=[
                pltpu.VMEM((tok_rows, width), BF16),
                pltpu.VMEM((1, width), F32),
                pltpu.VMEM((width, outw), BF16),
                pltpu.VMEM((tiles, K), jnp.int32),
                pltpu.VMEM((tiles, targets.shape[2]), BF16),
                pltpu.VMEM((group * cap, slots), BF16),
                pltpu.VMEM((packs, 1, 128), F32),
                pltpu.VMEM((group, 1, 128), F32),
                pltpu.VMEM((packs, PARAMS, 128), BF16),
                pltpu.VMEM((group, PARAMS, 128), BF16),
                pltpu.VMEM((group, tiles, K), jnp.int32),
                pltpu.VMEM((group // batch if ahead else 1, group * tok_rows, batch * slots), BF16),
                pltpu.VMEM((group, gpt, slots), BF16),
                pltpu.VMEM((group, tok_rows, width), BF16),
                pltpu.VMEM((group, 2 * PARAMS, slots // 2), BF16),
                pltpu.VMEM((2, ROWS * gpt, group * tok_rows), F32),
                pltpu.VMEM((nsec * nlo, width, group * tok_rows // (nsec * nlo)), BF16),
                pltpu.VMEM((nsec * nlo, width, group * tok_rows // (nsec * nlo)), BF16),
                pltpu.VMEM((outw, group * tok_rows), BF16),
                pltpu.VMEM((outw, group * tok_rows), BF16),
                pltpu.VMEM((group, 1, K), F32),
                pltpu.VMEM((8, K), F32),
                pltpu.VMEM((8, K), F32),
                dma((5,)),
                dma((3,)), dma((3,)),
                dma((15,)), dma((15,)),
                dma((2,)), dma((group,)),
                dma((2,)), dma((2,)),
                dma((2,)), dma,
                dma((nsec * nlo,)), dma((nsec * nlo,)),
            ],
            compiler_params=pltpu.CompilerParams(
                collective_id=0, has_side_effects=True, vmem_limit_bytes=61 * 1024 * 1024
            ),
        )(
            tokens[0], norm_gain[None], head_weight, tile_lists[0], tile_counts[0], cameras[0],
            targets[0],
        )
        image, grad, loss = pl.pallas_call(
            store,
            out_shape=tuple(
                jax.ShapeDtypeStruct(shape, dtype)
                for shape, dtype in ((image.shape, BF16), (grad.shape, F32), ((1, 1), F32))
            ),
            in_specs=[vmem] * 3,
            out_specs=(hbm,) * 3,
            scratch_shapes=[pltpu.VMEM((1, 1), F32), dma((3,))],
            compiler_params=pltpu.CompilerParams(vmem_limit_bytes=1024 * 1024),
        )(image, grad, loss)
        return image[None], grad, loss[0, 0]

    in_specs = (
        P("scene", ("section", "view"), None),
        P(),
        P(),
        P("scene", ("section", "view"), None),
        P("scene", ("section", "view")),
        P("scene", None, None),
        P("scene", ("section", "view"), None),
    )
    out_specs = (P("scene", ("section", "view"), None), P(), P())
    return jax.shard_map(body, mesh=mesh, in_specs=in_specs, out_specs=out_specs, check_vma=False)
```

```python
import functools

import jax
import jax.numpy as jnp
from jax import lax
from jax.experimental import pallas as pl
from jax.experimental.pallas import tpu as pltpu
from jax.sharding import PartitionSpec as P

PARAMS = 8
ROWS = 7
SIDE = 16
BATCH = 2
STORES = 1
FINISH = 0
LATE = 1
VIEWS = 2
MESH = pl.DeviceIdType.MESH
F32 = jnp.float32
BF16 = jnp.bfloat16
LOG2E = 1.4426950408889634
NN = (((1,), (0,)), ((), ()))
NT = (((1,), (1,)), ((), ()))
TN = (((0,), (0,)), ((), ()))


def mm(a, b, dims):
    return lax.dot_general(a, b, dims, preferred_element_type=F32)


def split(x):
    hi = x.astype(BF16)
    lo = (x - hi.astype(F32)).astype(BF16)
    return hi, lo


def sigmoid(x):
    return 1.0 / (1.0 + jnp.exp(-x))


def turn(a, k, n):
    if n & (n - 1):
        return lax.rem(a + k, n)
    if isinstance(k, int):
        bit = 1
        while bit < n:
            if k & bit:
                a = a + bit - 2 * bit * lax.rem(a // bit, 2)
            bit *= 2
        return a
    out, bit = 0, 1
    while bit < n:
        out = out + bit * lax.rem((a // bit) + (k // bit), 2)
        bit *= 2
    return out


def kernel(
    nsec, nview, factor,
    tok_hbm, gain_hbm, w_hbm, list_hbm, count_ref, cam_ref, want_hbm,
    image_ref, grad_ref, loss_ref,
    tok_ref, gain_ref, w_ref, list_ref, want_ref,
    perm, asked, wanted, found, given, lists, where, fits, norms, grads, dhead, turned, turned_far, mine, theirs,
    losses, loss_mine, loss_theirs,
    s_in, s_small, r_small, s_norm, r_norm, s_grad, r_grad, s_part, r_part, s_loss, r_loss, s_turn, r_turn,
):
    group = nsec * nview
    nlo = 2
    nhi = nview // nlo
    sec, view, scene = lax.axis_index("section"), lax.axis_index("view"), lax.axis_index("scene")
    hi, lo = view // nlo, lax.rem(view, nlo)
    me = sec * nview + view
    tok_rows, width = tok_ref.shape
    outw = w_ref.shape[1]
    gpt = outw // PARAMS
    tiles, K = list_ref.shape
    slots = tiles * K
    tokens = group * tok_rows
    pix = SIDE * SIDE
    cap = 2 * slots // group
    per = 128 // cap
    packs = group // per
    ahead = where.shape[0] > 1
    batch = where.shape[2] // slots

    def local(n, src, dst):
        return pltpu.make_async_copy(src, dst, s_in.at[n])

    loads = [
        local(0, list_hbm, list_ref),
        local(1, tok_hbm, tok_ref),
        local(2, gain_hbm, gain_ref),
        local(3, w_hbm, w_ref),
        local(4, want_hbm, want_ref),
    ]
    for load in loads:
        load.start()

    known = {}

    def each_peer(act):
        if group <= 16:
            for i in range(group - 1, 0, -1):
                act(i)
        else:
            pl.loop(1, group)(act)

    def peer(i):
        if isinstance(i, int):
            if i not in known:
                known[i] = find(i)
            return known[i]
        return find(i)

    def find(i):
        s = turn(sec, i % nsec, nsec)
        l = turn(lo, (i // nsec) % nlo, nlo)
        h = turn(hi, i // (nsec * nlo), nhi)
        v = h * nlo + l
        return s * nview + v, (s, v, scene)

    def place_of(s, l, h):
        return (s * nlo + l) * nhi + h

    partner = (sec, view, 1 - scene)
    barrier = pltpu.get_barrier_semaphore()

    @each_peer
    def _(i):
        pl.semaphore_signal(barrier, inc=1, device_id=peer(i)[1], device_id_type=MESH)

    pl.semaphore_signal(barrier, inc=1, device_id=partner, device_id_type=MESH)

    loads[0].wait()
    number = jnp.concatenate([list_ref[pl.ds(b, 1), :] for b in range(tiles)], axis=1)
    token = number // gpt
    gauss = number - token * gpt
    owner = token // tok_rows
    inner = token - owner * tok_rows
    ow_sec = owner // nview
    ow_hi = (owner - ow_sec * nview) // nlo
    ow_lo = owner - ow_sec * nview - ow_hi * nlo
    row = place_of(ow_sec, ow_lo, ow_hi) * tok_rows + inner
    code = row * gpt + gauss
    for b in range(tiles):
        lists[me, pl.ds(b, 1), :] = code[:, b * K : (b + 1) * K]
    mask = jnp.where(lax.broadcasted_iota(jnp.int32, (group, slots), 0) == owner, 1.0, 0.0)
    earlier = jnp.where(
        lax.broadcasted_iota(jnp.int32, (slots, slots), 0)
        < lax.broadcasted_iota(jnp.int32, (slots, slots), 1),
        1.0, 0.0,
    ).astype(BF16)
    rank = jnp.sum(mask * mm(mask.astype(BF16), earlier, NN), axis=0, keepdims=True)
    dest = owner * cap + rank.astype(jnp.int32)
    perm[...] = jnp.where(
        lax.broadcasted_iota(jnp.int32, (group * cap, slots), 0) == dest, 1.0, 0.0
    ).astype(BF16)
    asks = jnp.concatenate(
        [inner.astype(F32), gauss.astype(F32), jnp.zeros((6, slots), F32)], axis=0
    ).astype(BF16)
    requests = mm(asks, perm[...], NT)
    requests = requests[0:1] * float(gpt) + requests[1:2]
    for i in range(packs):
        asked[i] = requests[:, i * 128 : (i + 1) * 128]
    wanted[me] = asked[me // per]

    pl.semaphore_wait(barrier, group)

    def small(n, src, dst, where_to):
        return pltpu.make_async_remote_copy(
            src_ref=src, dst_ref=dst, send_sem=s_small.at[n], recv_sem=r_small.at[n],
            device_id=where_to, device_id_type=MESH,
        )

    def all_small(n, buf):
        span = buf.at[pl.ds(0, group - 1)]
        return small(n, span, span, partner)

    @each_peer
    def _(i):
        j, to = peer(i)
        small(0, asked.at[j // per], wanted.at[me], to).start()

    @each_peer
    def _(i):
        small(1, lists.at[me], lists.at[me], peer(i)[1]).start()

    loads[1].wait()
    loads[2].wait()
    spot = place_of(sec, lo, hi)
    x = tok_ref[...].astype(F32)
    scale = lax.rsqrt(jnp.mean(x * x, axis=-1, keepdims=True) + 1e-06)
    normed = (x * scale * gain_ref[...]).astype(BF16)
    norms[spot] = normed

    def block(s, l, k):
        return place_of(s, l, turn(hi, k, nhi))

    half = tok_rows // 2
    parts = {"whole": pl.ds(0, tok_rows), "top": pl.ds(0, half), "bottom": pl.ds(half, half)}
    classes = [[0], [1], list(range(2, nhi))]
    beside = (1 - sec, view, scene)
    below = (sec, hi * nlo + 1 - lo, scene)

    def norm_copy(n, ref, to):
        return pltpu.make_async_remote_copy(
            src_ref=ref, dst_ref=ref, send_sem=s_norm, recv_sem=r_norm.at[n],
            device_id=to, device_id_type=MESH,
        )

    flows = {
        "x": (3, beside, sec, lo, "whole"),
        "y": (6, below, sec, lo, "whole"),
        "far_x": (9, beside, sec, 1 - lo, "top"),
        "far_y": (12, below, 1 - sec, lo, "bottom"),
    }

    def line_send(c):
        for k in classes[c]:
            to = (sec, turn(hi, k, nhi) * nlo + lo, scene)
            norm_copy(c, norms.at[block(sec, lo, 0)], to).start()

    def flow_send(name, c):
        n, to, s, l, part = flows[name]
        for k in classes[c]:
            norm_copy(n + c, norms.at[block(s, l, k), parts[part]], to).start()

    def flow_all(name, c):
        n, _, _, _, part = flows[name]
        return norm_copy(n + c, norms.at[pl.ds(0, len(classes[c])), parts[part]], partner)

    def line_all(c):
        return norm_copy(c, norms.at[pl.ds(0, len(classes[c]))], partner)

    line_send(1)
    flow_send("x", 0)
    flow_send("y", 0)
    line_send(2)

    loads[3].wait()
    head = mm(normed, w_ref[...], NN)
    stack = jnp.concatenate(
        [head[:, p * gpt : (p + 1) * gpt] for p in range(PARAMS)], axis=0
    ).astype(BF16)
    er = lax.broadcasted_iota(jnp.int32, (PARAMS * tok_rows, PARAMS * tok_rows), 0)
    ec = lax.broadcasted_iota(jnp.int32, (PARAMS * tok_rows, PARAMS * tok_rows), 1)
    swap = jnp.where(ec == (er % PARAMS) * tok_rows + er // PARAMS, 1.0, 0.0).astype(BF16)
    table = mm(swap, stack, NN).astype(BF16)

    lane = lax.broadcasted_iota(jnp.int32, (8, 128), 1)
    mine_at = lax.rem(me, per)

    def gathered(buf):
        out = []
        for i in range(packs):
            total = None
            for k in range(per):
                q = lax.rem(mine_at + k, per)
                block = buf[i * per + q].astype(F32)
                if k:
                    block = pltpu.roll(block, k * cap, 1)
                total = block if total is None else jnp.where(lane[: block.shape[0]] // cap == q, block, total)
            out.append(total)
        return jnp.concatenate(out, axis=1)

    all_small(0, wanted).wait_recv()
    asks_in = gathered(wanted)
    ask = asks_in.astype(jnp.int32)
    ask_t = ask // gpt
    ask_g = ask - ask_t * gpt
    hot = jnp.where(
        lax.broadcasted_iota(jnp.int32, (gpt, group * cap), 0) == ask_g, 1.0, 0.0
    ).astype(BF16)
    spread_rows = mm(table, hot, NN)
    answer = jnp.zeros((PARAMS, group * cap), F32)
    for t in range(tok_rows):
        answer = jnp.where(
            ask_t == t, spread_rows[t * PARAMS : (t + 1) * PARAMS], answer
        )
    for i in range(packs):
        found[i] = answer[:, i * 128 : (i + 1) * 128].astype(BF16)
    given[me] = found[me // per]

    @each_peer
    def _(i):
        j, to = peer(i)
        small(2, found.at[j // per], given.at[me], to).start()

    stretch = nhi * tok_rows

    def turn_copy(s, l):
        n = s * nlo + l
        return pltpu.make_async_remote_copy(
            src_ref=turned.at[n], dst_ref=turned_far.at[n], send_sem=s_turn,
            recv_sem=r_turn, device_id=partner, device_id_type=MESH,
        )

    def turn_line(s, l):
        n = s * nlo + l
        turned[n] = norms[pl.ds(n * nhi, nhi)].reshape(stretch, width).T
        turn_copy(s, l).start()

    line_all(1).wait_recv()
    flow_send("x", 1)
    flow_send("y", 1)
    flow_all("x", 0).wait_recv()
    flow_all("y", 0).wait_recv()
    flow_send("far_x", 0)
    flow_send("far_y", 0)
    all_small(1, lists).wait_recv()
    row_at = lax.broadcasted_iota(jnp.int32, (tokens, K), 0)
    gauss_at = lax.broadcasted_iota(jnp.int32, (gpt, K), 0)

    def source(g, q):
        return (g // 2) * (2 * batch) + g % 2 + 2 * q

    def mark_rows(g, n):
        for q in range(batch):
            j = peer(source(g, q))[0]
            for b in range(tiles):
                at = lists[j, pl.ds(b, 1), :] // gpt
                where[n, :, (q * tiles + b) * K : (q * tiles + b + 1) * K] = jnp.where(
                    row_at == at, 1.0, 0.0
                ).astype(BF16)

    @pl.loop(0, group // batch)
    def _(g):
        if ahead:
            mark_rows(g, g)

    @pl.loop(0, group)
    def _(j):
        for b in range(tiles):
            at = lists[j, pl.ds(b, 1), :]
            at = at - (at // gpt) * gpt
            fits[j, :, b * K : (b + 1) * K] = jnp.where(gauss_at == at, 1.0, 0.0).astype(BF16)

    line_all(2).wait_recv()
    flow_send("x", 2)
    flow_send("y", 2)
    flow_all("x", 1).wait_recv()
    flow_all("y", 1).wait_recv()
    flow_send("far_x", 1)
    flow_send("far_y", 1)
    turn_line(sec, lo)
    all_small(2, given).wait_recv()
    picked = mm(gathered(given).astype(BF16), perm[...], NN)
    rows = [picked[p : p + 1] for p in range(PARAMS)]
    loads[4].wait()

    place = lax.broadcasted_iota(jnp.int32, (1, pix), 1)
    across = ((place % SIDE).astype(F32) + 0.5) * (2.0 / SIDE) - 1.0
    down = ((place // SIDE).astype(F32) + 0.5) * (2.0 / SIDE) - 1.0
    ka = lax.broadcasted_iota(jnp.int32, (K, 2 * K), 0)
    kb = lax.rem(lax.broadcasted_iota(jnp.int32, (K, 2 * K), 1), K)
    lower = jnp.where(kb < ka, 1.0, 0.0).astype(BF16)
    upper = jnp.where(kb > ka, 1.0, 0.0).astype(BF16)
    moments = jnp.concatenate(
        [jnp.ones((1, pix), F32), across, down, across * across + down * down, jnp.zeros((4, pix), F32)],
        axis=0,
    ).astype(BF16)
    cam = [cam_ref[sec, n] for n in range(8)]
    cam_far = [cam_ref[1 - sec, n] for n in range(8)]
    slot = lax.broadcasted_iota(jnp.int32, (1, K), 1)
    live = jnp.concatenate(
        [jnp.where(slot < count_ref[b], 1.0, 0.0) for b in range(tiles)], axis=1
    )
    mx, my, mz, ls, op = rows[:5]
    sx = jnp.tanh(cam[0] * mx + cam[1] * my + cam[2] * mz + cam[3])
    sy = jnp.tanh(cam[4] * mx + cam[5] * my + cam[6] * mz + cam[7])
    spread = jnp.exp(-2.0 * ls)
    sop = sigmoid(op)
    amp = 0.3 * sop * live
    shade = sigmoid(picked[5:8])
    shade8 = jnp.concatenate([shade, jnp.zeros((5, slots), F32)], axis=0)
    steep = (-0.5 * LOG2E) * jnp.minimum(spread, 1e38)
    cols = jnp.concatenate([sx, sy, steep, amp, jnp.zeros((4, slots), F32)], axis=0).T
    cuts = [slice(b * K, (b + 1) * K) for b in range(tiles)]

    alphas, inverses, logs = [], [], []
    for cut in cuts:
        csx, csy, csp, camp = [cols[cut, n : n + 1] for n in range(4)]
        dx = across - csx
        dy = down - csy
        alpha = camp * jnp.exp2((dx * dx + dy * dy) * csp)
        rest = 1.0 - alpha
        alphas.append(alpha)
        inverses.append(alpha / rest)
        logs.append(jnp.concatenate(split(jnp.log(rest)), axis=0))
    befores = [mm(lower, x, NN) for x in logs]
    weights = [alpha * jnp.exp(before) for alpha, before in zip(alphas, befores)]
    packed = [weight.astype(BF16) for weight in weights]
    shade_hi, shade_lo = split(shade8)
    shade_two = jnp.concatenate([shade_hi, shade_lo], axis=0)
    colours = []
    for cut, weight in zip(cuts, packed):
        both = mm(shade_two[:, cut], weight, NN)
        colours.append(both[:8] + both[8:])
    loss_part = jnp.zeros((1, K), F32)
    dcols = []
    for b in range(tiles):
        want = jnp.concatenate(
            [want_ref[pl.ds(b, 1), c * pix : (c + 1) * pix].astype(F32) for c in range(3)]
            + [jnp.zeros((5, pix), F32)],
            axis=0,
        )
        for c in range(3):
            image_ref[pl.ds(b, 1), c * pix : (c + 1) * pix] = colours[b][c : c + 1].astype(BF16)
        diff = colours[b] - want
        sq = jnp.sum(diff * diff, axis=0, keepdims=True)
        for n in range(0, pix, K):
            loss_part = loss_part + sq[:, n : n + K]
        dcols.append(((2.0 * factor) * diff).astype(BF16))
    losses[me] = loss_part * factor
    dshade = jnp.concatenate([mm(d, w, NT) for d, w in zip(dcols, packed)], axis=1)
    dwws = [
        mm(shade_hi[:, cut], d, TN) * weight for cut, d, weight in zip(cuts, dcols, weights)
    ]
    dlogs = [mm(upper[:, :K], x.astype(BF16), NN) for x in dwws]
    sums = []
    for x, y, inverse in zip(dwws, dlogs, inverses):
        h = x - y * inverse
        both = mm(moments, jnp.concatenate(split(h), axis=0), NT)
        sums.append(both[:, :K] + both[:, K:])
    sums = jnp.concatenate(sums, axis=1)
    s_h, s_u, s_v, s_q = [sums[n : n + 1] for n in range(4)]
    s_x = s_u - sx * s_h
    s_y = s_v - sy * s_h
    s_r = s_q - 2.0 * (sx * s_u + sy * s_v) + (sx * sx + sy * sy) * s_h
    px = spread * s_x * (1.0 - sx * sx)
    py = spread * s_y * (1.0 - sy * sy)
    out = jnp.concatenate(
        [
            px,
            py,
            spread * s_r,
            (1.0 - sop) * s_h,
            dshade[0:3] * shade * (1.0 - shade),
            jnp.zeros((1, slots), F32),
        ],
        axis=0,
    )
    wide = slots // 2
    grads[me] = jnp.concatenate([out[:, :wide], out[:, wide:]], axis=0).astype(BF16)

    def push(n, buf, i, recv):
        j, to = peer(i)
        return pltpu.make_async_remote_copy(
            src_ref=buf.at[me], dst_ref=buf.at[me], send_sem=s_grad.at[n],
            recv_sem=recv, device_id=to, device_id_type=MESH,
        )

    @each_peer
    def _(i):
        push(0, grads, i, r_grad.at[me]).start()

    flow_all("x", 2).wait_recv()
    flow_all("y", 2).wait_recv()
    turn_line(1 - sec, lo)
    turn_line(sec, 1 - lo)

    def late_sends():
        flow_send("far_x", 2)
        flow_send("far_y", 2)

        @each_peer
        def _(i):
            push(1, losses, i, s_loss.at[1]).start()

    def gather_batch(g, n):
        sides = []
        for q in range(batch):
            i = source(g, q)
            j = peer(i)[0]
            if isinstance(i, int):
                if i > 0:
                    push(0, grads, i, r_grad.at[j]).wait_recv()
            else:
                pl.when(i > 0)(lambda: push(0, grads, i, r_grad.at[j]).wait_recv())
            got = grads[j]
            fit = fits[j]
            sides.append(
                jnp.concatenate(
                    [
                        jnp.concatenate(
                            [
                                fit[:, :wide] * got[p : p + 1],
                                fit[:, wide:] * got[PARAMS + p : PARAMS + p + 1],
                            ],
                            axis=1,
                        )
                        for p in range(ROWS)
                    ],
                    axis=0,
                )
            )
        return mm(jnp.concatenate(sides, axis=1), where[n], NT)

    def finish_turning():
        for name in ("far_x", "far_y"):
            for c in range(3):
                flow_all(name, c).wait_recv()
        turn_line(1 - sec, 1 - lo)

    last = group // batch - 1
    if ahead:
        for g in range(last + 1):
            if g == LATE:
                late_sends()
            if g == last + FINISH:
                finish_turning()
            if g < 2:
                dhead[g] = gather_batch(g, g)
            else:
                dhead[g % 2] += gather_batch(g, g)
        if FINISH > 0:
            finish_turning()
    else:
        late_sends()
        dhead[...] = jnp.zeros_like(dhead)

        @pl.loop(0, last + 1)
        def _(g):
            mark_rows(g, 0)
            dhead[g % 2] += gather_batch(g, 0)

        finish_turning()

    loss_all = losses.at[pl.ds(0, group - 1)]
    pltpu.make_async_remote_copy(
        src_ref=loss_all, dst_ref=loss_all, send_sem=s_grad.at[1], recv_sem=s_loss.at[1],
        device_id=partner, device_id_type=MESH,
    ).wait_recv()
    loss_mine[...] = jnp.broadcast_to(jnp.sum(losses[...], axis=0), loss_mine.shape)
    loss_copy = pltpu.make_async_remote_copy(
        src_ref=loss_mine, dst_ref=loss_theirs, send_sem=s_loss.at[0], recv_sem=r_loss,
        device_id=partner, device_id_type=MESH,
    )
    chunk = outw // 2
    dhead_rows = 256
    chunks = width // dhead_rows

    def part_copy(c):
        span = pl.ds(c * chunk, chunk)
        return pltpu.make_async_remote_copy(
            src_ref=mine.at[span], dst_ref=theirs.at[span],
            send_sem=s_part.at[c], recv_sem=r_part.at[c],
            device_id=partner, device_id_type=MESH,
        )

    def share(v, n):
        return dhead[v, n * gpt : (n + 1) * gpt]

    for p in [4, 5, 6, 7, 0, 1, 2, 3]:
        if p < 3:
            value = (
                cam[p] * share(0, 0) + cam[p + 4] * share(0, 1)
                + cam_far[p] * share(1, 0) + cam_far[p + 4] * share(1, 1)
            )
        else:
            value = share(0, p - 1) + share(1, p - 1)
        mine[p * gpt : (p + 1) * gpt] = value.astype(BF16)
        if (p + 1) * gpt % chunk == 0:
            part_copy((p + 1) * gpt // chunk - 1).start()
    loss_copy.start()

    def sides(buf, n):
        span = slice(n * dhead_rows, (n + 1) * dhead_rows)
        return span, jnp.concatenate([buf[m, span] for m in range(nsec * nlo)], axis=1)

    dh = mine[...]
    for n in range(chunks):
        span, side = sides(turned, n)
        grad_ref[span, :] = mm(side, dh, NT)
    turn_all = pltpu.make_async_remote_copy(
        src_ref=turned, dst_ref=turned_far, send_sem=s_turn, recv_sem=r_turn,
        device_id=partner, device_id_type=MESH,
    )
    turn_all.wait_recv()
    for c in (1, 0):
        part_copy(c).wait_recv()
        cut = slice(c * chunk, (c + 1) * chunk)
        dh = theirs[cut]
        for n in range(chunks):
            span, side = sides(turned_far, n)
            grad_ref[span, cut] += mm(side, dh, NT)
    loss_copy.wait_recv()
    loss_ref[...] = jnp.broadcast_to(
        jnp.sum(loss_mine[0:1] + loss_theirs[0:1], keepdims=True), loss_ref.shape
    )

    loss_copy.wait_send()
    for c in range(2):
        part_copy(c).wait_send()
    turn_all.wait_send()
    all_small(0, wanted).wait_send()
    all_small(1, lists).wait_send()
    all_small(2, given).wait_send()
    grad_all = grads.at[pl.ds(0, group - 1)]
    pltpu.make_async_remote_copy(
        src_ref=grad_all, dst_ref=grad_all, send_sem=s_grad.at[0], recv_sem=r_grad.at[0],
        device_id=partner, device_id_type=MESH,
    ).wait_send()
    pltpu.make_async_remote_copy(
        src_ref=loss_all, dst_ref=loss_all, send_sem=s_grad.at[1], recv_sem=s_loss.at[1],
        device_id=partner, device_id_type=MESH,
    ).wait_send()
    norm_copy(0, norms.at[pl.ds(0, group - 1)], partner).wait_send()


def store(image_ref, grad_ref, loss_ref, image_out, grad_out, loss_out, one, sems):
    rows = grad_ref.shape[0] // STORES
    pairs = [(image_ref, image_out), (one, loss_out)]
    for n in range(STORES):
        span = pl.ds(n * rows, rows)
        pairs.append((grad_ref.at[span], grad_out.at[span]))
    copies = [pltpu.make_async_copy(src, dst, sems.at[n]) for n, (src, dst) in enumerate(pairs)]
    one[...] = loss_ref[0:1, 0:1]
    for copy in copies:
        copy.start()
    for copy in copies:
        copy.wait()


def solution(mesh):
    nsec, nview, nscene = mesh.shape["section"], mesh.shape["view"], mesh.shape["scene"]
    group = nsec * nview
    nlo = 2
    assert nsec == 2 and nview % 8 == 0

    def body(tokens, norm_gain, head_weight, tile_lists, tile_counts, cameras, targets):
        tok_rows, width = tokens.shape[1:]
        outw = head_weight.shape[1]
        gpt = outw // PARAMS
        tiles, K = tile_lists.shape[1:]
        slots = tiles * K
        cap = 2 * slots // group
        packs = group * cap // 128
        factor = 1.0 / (nscene * tiles * group)
        ahead = group * group * tok_rows * slots <= 2**24
        batch = min(BATCH, group)
        vmem = pl.BlockSpec(memory_space=pltpu.VMEM)
        smem = pl.BlockSpec(memory_space=pltpu.SMEM)
        hbm = pl.BlockSpec(memory_space=pltpu.HBM)
        dma = pltpu.SemaphoreType.DMA
        image, grad, loss = pl.pallas_call(
            functools.partial(kernel, nsec, nview, factor),
            out_shape=(
                pltpu.VMEM((tiles, targets.shape[2]), BF16),
                pltpu.VMEM((width, outw), F32),
                pltpu.VMEM((8, 128), F32),
            ),
            in_specs=[hbm, hbm, hbm, hbm, smem, smem, hbm],
            out_specs=(vmem, vmem, vmem),
            scratch_shapes=[
                pltpu.VMEM((tok_rows, width), BF16),
                pltpu.VMEM((1, width), F32),
                pltpu.VMEM((width, outw), BF16),
                pltpu.VMEM((tiles, K), jnp.int32),
                pltpu.VMEM((tiles, targets.shape[2]), BF16),
                pltpu.VMEM((group * cap, slots), BF16),
                pltpu.VMEM((packs, 1, 128), F32),
                pltpu.VMEM((group, 1, 128), F32),
                pltpu.VMEM((packs, PARAMS, 128), BF16),
                pltpu.VMEM((group, PARAMS, 128), BF16),
                pltpu.VMEM((group, tiles, K), jnp.int32),
                pltpu.VMEM((group // batch if ahead else 1, group * tok_rows, batch * slots), BF16),
                pltpu.VMEM((group, gpt, slots), BF16),
                pltpu.VMEM((group, tok_rows, width), BF16),
                pltpu.VMEM((group, 2 * PARAMS, slots // 2), BF16),
                pltpu.VMEM((2, ROWS * gpt, group * tok_rows), F32),
                pltpu.VMEM((nsec * nlo, width, group * tok_rows // (nsec * nlo)), BF16),
                pltpu.VMEM((nsec * nlo, width, group * tok_rows // (nsec * nlo)), BF16),
                pltpu.VMEM((outw, group * tok_rows), BF16),
                pltpu.VMEM((outw, group * tok_rows), BF16),
                pltpu.VMEM((group, 1, K), F32),
                pltpu.VMEM((8, K), F32),
                pltpu.VMEM((8, K), F32),
                dma((5,)),
                dma((3,)), dma((3,)),
                dma, dma((15,)),
                dma((2,)), dma((group,)),
                dma((2,)), dma((2,)),
                dma((2,)), dma,
                dma, dma,
            ],
            compiler_params=pltpu.CompilerParams(
                collective_id=0, has_side_effects=True, vmem_limit_bytes=61 * 1024 * 1024
            ),
        )(
            tokens[0], norm_gain[None], head_weight, tile_lists[0], tile_counts[0], cameras[0],
            targets[0],
        )
        image, grad, loss = pl.pallas_call(
            store,
            out_shape=tuple(
                jax.ShapeDtypeStruct(shape, dtype)
                for shape, dtype in ((image.shape, BF16), (grad.shape, F32), ((1, 1), F32))
            ),
            in_specs=[vmem] * 3,
            out_specs=(hbm,) * 3,
            scratch_shapes=[pltpu.VMEM((1, 1), F32), dma((2 + STORES,))],
            compiler_params=pltpu.CompilerParams(vmem_limit_bytes=1024 * 1024),
        )(image, grad, loss)
        return image[None], grad, loss[0, 0]

    in_specs = (
        P("scene", ("section", "view"), None),
        P(),
        P(),
        P("scene", ("section", "view"), None),
        P("scene", ("section", "view")),
        P("scene", None, None),
        P("scene", ("section", "view"), None),
    )
    out_specs = (P("scene", ("section", "view"), None), P(), P())
    return jax.shard_map(body, mesh=mesh, in_specs=in_specs, out_specs=out_specs, check_vma=False)
```

```python
import functools

import jax
import jax.numpy as jnp
from jax import lax
from jax.experimental import pallas as pl
from jax.experimental.pallas import tpu as pltpu
from jax.sharding import PartitionSpec as P

PARAMS = 8
ROWS = 7
SIDE = 16
BATCH = 2
STORES = 1
FINISH = 0
LATE = 0
VIEWS = 2
MESH = pl.DeviceIdType.MESH
F32 = jnp.float32
BF16 = jnp.bfloat16
LOG2E = 1.4426950408889634
NN = (((1,), (0,)), ((), ()))
NT = (((1,), (1,)), ((), ()))
TN = (((0,), (0,)), ((), ()))


def mm(a, b, dims):
    return lax.dot_general(a, b, dims, preferred_element_type=F32)


def split(x):
    hi = x.astype(BF16)
    lo = (x - hi.astype(F32)).astype(BF16)
    return hi, lo


def sigmoid(x):
    return 1.0 / (1.0 + jnp.exp(-x))


def turn(a, k, n):
    if n & (n - 1):
        return lax.rem(a + k, n)
    if isinstance(k, int):
        bit = 1
        while bit < n:
            if k & bit:
                a = a + bit - 2 * bit * lax.rem(a // bit, 2)
            bit *= 2
        return a
    out, bit = 0, 1
    while bit < n:
        out = out + bit * lax.rem((a // bit) + (k // bit), 2)
        bit *= 2
    return out


def kernel(
    nsec, nview, factor,
    tok_hbm, gain_hbm, w_hbm, list_hbm, count_ref, cam_ref, want_hbm,
    image_ref, grad_ref, loss_ref,
    tok_ref, gain_ref, w_ref, list_ref, want_ref,
    perm, asked, wanted, found, given, lists, where, fits, norms, grads, dhead, turned, turned_far, mine, theirs,
    losses, loss_mine, loss_theirs,
    s_in, s_small, r_small, s_norm, r_norm, s_grad, r_grad, s_part, r_part, s_loss, r_loss, s_turn, r_turn,
):
    group = nsec * nview
    nlo = 2
    nhi = nview // nlo
    sec, view, scene = lax.axis_index("section"), lax.axis_index("view"), lax.axis_index("scene")
    hi, lo = view // nlo, lax.rem(view, nlo)
    me = sec * nview + view
    tok_rows, width = tok_ref.shape
    outw = w_ref.shape[1]
    gpt = outw // PARAMS
    tiles, K = list_ref.shape
    slots = tiles * K
    tokens = group * tok_rows
    pix = SIDE * SIDE
    cap = 2 * slots // group
    per = 128 // cap
    packs = group // per
    ahead = where.shape[0] > 1
    batch = where.shape[2] // slots

    def local(n, src, dst):
        return pltpu.make_async_copy(src, dst, s_in.at[n])

    loads = [
        local(0, list_hbm, list_ref),
        local(1, tok_hbm, tok_ref),
        local(2, gain_hbm, gain_ref),
        local(3, w_hbm, w_ref),
        local(4, want_hbm, want_ref),
    ]
    for load in loads:
        load.start()

    known = {}

    def each_peer(act):
        if group <= 16:
            for i in range(group - 1, 0, -1):
                act(i)
        else:
            pl.loop(1, group)(act)

    def peer(i):
        if isinstance(i, int):
            if i not in known:
                known[i] = find(i)
            return known[i]
        return find(i)

    def find(i):
        s = turn(sec, i % nsec, nsec)
        l = turn(lo, (i // nsec) % nlo, nlo)
        h = turn(hi, i // (nsec * nlo), nhi)
        v = h * nlo + l
        return s * nview + v, (s, v, scene)

    def place_of(s, l, h):
        return (s * nlo + l) * nhi + h

    partner = (sec, view, 1 - scene)
    barrier = pltpu.get_barrier_semaphore()

    @each_peer
    def _(i):
        pl.semaphore_signal(barrier, inc=1, device_id=peer(i)[1], device_id_type=MESH)

    pl.semaphore_signal(barrier, inc=1, device_id=partner, device_id_type=MESH)

    loads[0].wait()
    number = jnp.concatenate([list_ref[pl.ds(b, 1), :] for b in range(tiles)], axis=1)
    token = number // gpt
    gauss = number - token * gpt
    owner = token // tok_rows
    inner = token - owner * tok_rows
    ow_sec = owner // nview
    ow_hi = (owner - ow_sec * nview) // nlo
    ow_lo = owner - ow_sec * nview - ow_hi * nlo
    row = place_of(ow_sec, ow_lo, ow_hi) * tok_rows + inner
    code = row * gpt + gauss
    for b in range(tiles):
        lists[me, pl.ds(b, 1), :] = code[:, b * K : (b + 1) * K]
    mask = jnp.where(lax.broadcasted_iota(jnp.int32, (group, slots), 0) == owner, 1.0, 0.0)
    earlier = jnp.where(
        lax.broadcasted_iota(jnp.int32, (slots, slots), 0)
        < lax.broadcasted_iota(jnp.int32, (slots, slots), 1),
        1.0, 0.0,
    ).astype(BF16)
    rank = jnp.sum(mask * mm(mask.astype(BF16), earlier, NN), axis=0, keepdims=True)
    dest = owner * cap + rank.astype(jnp.int32)
    perm[...] = jnp.where(
        lax.broadcasted_iota(jnp.int32, (group * cap, slots), 0) == dest, 1.0, 0.0
    ).astype(BF16)
    asks = jnp.concatenate(
        [inner.astype(F32), gauss.astype(F32), jnp.zeros((6, slots), F32)], axis=0
    ).astype(BF16)
    requests = mm(asks, perm[...], NT)
    requests = requests[0:1] * float(gpt) + requests[1:2]
    for i in range(packs):
        asked[i] = requests[:, i * 128 : (i + 1) * 128]
    wanted[me] = asked[me // per]

    pl.semaphore_wait(barrier, group)

    def small(n, src, dst, where_to):
        return pltpu.make_async_remote_copy(
            src_ref=src, dst_ref=dst, send_sem=s_small.at[n], recv_sem=r_small.at[n],
            device_id=where_to, device_id_type=MESH,
        )

    def all_small(n, buf):
        span = buf.at[pl.ds(0, group - 1)]
        return small(n, span, span, partner)

    @each_peer
    def _(i):
        j, to = peer(i)
        small(0, asked.at[j // per], wanted.at[me], to).start()

    @each_peer
    def _(i):
        small(1, lists.at[me], lists.at[me], peer(i)[1]).start()

    loads[1].wait()
    loads[2].wait()
    spot = place_of(sec, lo, hi)
    x = tok_ref[...].astype(F32)
    scale = lax.rsqrt(jnp.mean(x * x, axis=-1, keepdims=True) + 1e-06)
    normed = (x * scale * gain_ref[...]).astype(BF16)
    norms[spot] = normed

    def block(s, l, k):
        return place_of(s, l, turn(hi, k, nhi))

    half = tok_rows // 2
    parts = {"whole": pl.ds(0, tok_rows), "top": pl.ds(0, half), "bottom": pl.ds(half, half)}
    classes = [[0], [1], list(range(2, nhi))]
    beside = (1 - sec, view, scene)
    below = (sec, hi * nlo + 1 - lo, scene)

    def norm_copy(n, ref, to):
        return pltpu.make_async_remote_copy(
            src_ref=ref, dst_ref=ref, send_sem=s_norm, recv_sem=r_norm.at[n],
            device_id=to, device_id_type=MESH,
        )

    flows = {
        "x": (3, beside, sec, lo, "whole"),
        "y": (6, below, sec, lo, "whole"),
        "far_x": (9, beside, sec, 1 - lo, "top"),
        "far_y": (12, below, 1 - sec, lo, "bottom"),
    }

    def line_send(c):
        for k in classes[c]:
            to = (sec, turn(hi, k, nhi) * nlo + lo, scene)
            norm_copy(c, norms.at[block(sec, lo, 0)], to).start()

    def flow_send(name, c):
        n, to, s, l, part = flows[name]
        for k in classes[c]:
            norm_copy(n + c, norms.at[block(s, l, k), parts[part]], to).start()

    def flow_all(name, c):
        n, _, _, _, part = flows[name]
        return norm_copy(n + c, norms.at[pl.ds(0, len(classes[c])), parts[part]], partner)

    def line_all(c):
        return norm_copy(c, norms.at[pl.ds(0, len(classes[c]))], partner)

    line_send(1)
    flow_send("x", 0)
    flow_send("y", 0)
    line_send(2)

    loads[3].wait()
    head = mm(normed, w_ref[...], NN)
    stack = jnp.concatenate(
        [head[:, p * gpt : (p + 1) * gpt] for p in range(PARAMS)], axis=0
    ).astype(BF16)
    er = lax.broadcasted_iota(jnp.int32, (PARAMS * tok_rows, PARAMS * tok_rows), 0)
    ec = lax.broadcasted_iota(jnp.int32, (PARAMS * tok_rows, PARAMS * tok_rows), 1)
    swap = jnp.where(ec == (er % PARAMS) * tok_rows + er // PARAMS, 1.0, 0.0).astype(BF16)
    table = mm(swap, stack, NN).astype(BF16)

    lane = lax.broadcasted_iota(jnp.int32, (8, 128), 1)
    mine_at = lax.rem(me, per)

    def gathered(buf):
        out = []
        for i in range(packs):
            total = None
            for k in range(per):
                q = lax.rem(mine_at + k, per)
                block = buf[i * per + q].astype(F32)
                if k:
                    block = pltpu.roll(block, k * cap, 1)
                total = block if total is None else jnp.where(lane[: block.shape[0]] // cap == q, block, total)
            out.append(total)
        return jnp.concatenate(out, axis=1)

    all_small(0, wanted).wait_recv()
    asks_in = gathered(wanted)
    ask = asks_in.astype(jnp.int32)
    ask_t = ask // gpt
    ask_g = ask - ask_t * gpt
    hot = jnp.where(
        lax.broadcasted_iota(jnp.int32, (gpt, group * cap), 0) == ask_g, 1.0, 0.0
    ).astype(BF16)
    spread_rows = mm(table, hot, NN)
    answer = jnp.zeros((PARAMS, group * cap), F32)
    for t in range(tok_rows):
        answer = jnp.where(
            ask_t == t, spread_rows[t * PARAMS : (t + 1) * PARAMS], answer
        )
    for i in range(packs):
        found[i] = answer[:, i * 128 : (i + 1) * 128].astype(BF16)
    given[me] = found[me // per]

    @each_peer
    def _(i):
        j, to = peer(i)
        small(2, found.at[j // per], given.at[me], to).start()

    stretch = nhi * tok_rows

    def turn_copy(s, l):
        n = s * nlo + l
        return pltpu.make_async_remote_copy(
            src_ref=turned.at[n], dst_ref=turned_far.at[n], send_sem=s_turn,
            recv_sem=r_turn, device_id=partner, device_id_type=MESH,
        )

    def turn_line(s, l):
        n = s * nlo + l
        turned[n] = norms[pl.ds(n * nhi, nhi)].reshape(stretch, width).T
        turn_copy(s, l).start()

    line_all(1).wait_recv()
    flow_send("x", 1)
    flow_send("y", 1)
    flow_all("x", 0).wait_recv()
    flow_all("y", 0).wait_recv()
    flow_send("far_x", 0)
    flow_send("far_y", 0)
    all_small(1, lists).wait_recv()
    row_at = lax.broadcasted_iota(jnp.int32, (tokens, K), 0)
    gauss_at = lax.broadcasted_iota(jnp.int32, (gpt, K), 0)

    def source(g, q):
        return (g // 2) * (2 * batch) + g % 2 + 2 * q

    def mark_rows(g, n):
        for q in range(batch):
            j = peer(source(g, q))[0]
            for b in range(tiles):
                at = lists[j, pl.ds(b, 1), :] // gpt
                where[n, :, (q * tiles + b) * K : (q * tiles + b + 1) * K] = jnp.where(
                    row_at == at, 1.0, 0.0
                ).astype(BF16)

    @pl.loop(0, group // batch)
    def _(g):
        if ahead:
            mark_rows(g, g)

    @pl.loop(0, group)
    def _(j):
        for b in range(tiles):
            at = lists[j, pl.ds(b, 1), :]
            at = at - (at // gpt) * gpt
            fits[j, :, b * K : (b + 1) * K] = jnp.where(gauss_at == at, 1.0, 0.0).astype(BF16)

    line_all(2).wait_recv()
    flow_send("x", 2)
    flow_send("y", 2)
    flow_all("x", 1).wait_recv()
    flow_all("y", 1).wait_recv()
    flow_send("far_x", 1)
    flow_send("far_y", 1)
    turn_line(sec, lo)
    all_small(2, given).wait_recv()
    picked = mm(gathered(given).astype(BF16), perm[...], NN)
    rows = [picked[p : p + 1] for p in range(PARAMS)]
    loads[4].wait()

    place = lax.broadcasted_iota(jnp.int32, (1, pix), 1)
    across = ((place % SIDE).astype(F32) + 0.5) * (2.0 / SIDE) - 1.0
    down = ((place // SIDE).astype(F32) + 0.5) * (2.0 / SIDE) - 1.0
    ka = lax.broadcasted_iota(jnp.int32, (K, 2 * K), 0)
    kb = lax.rem(lax.broadcasted_iota(jnp.int32, (K, 2 * K), 1), K)
    lower = jnp.where(kb < ka, 1.0, 0.0).astype(BF16)
    upper = jnp.where(kb > ka, 1.0, 0.0).astype(BF16)
    moments = jnp.concatenate(
        [jnp.ones((1, pix), F32), across, down, across * across + down * down, jnp.zeros((4, pix), F32)],
        axis=0,
    ).astype(BF16)
    cam = [cam_ref[sec, n] for n in range(8)]
    cam_far = [cam_ref[1 - sec, n] for n in range(8)]
    slot = lax.broadcasted_iota(jnp.int32, (1, K), 1)
    live = jnp.concatenate(
        [jnp.where(slot < count_ref[b], 1.0, 0.0) for b in range(tiles)], axis=1
    )
    mx, my, mz, ls, op = rows[:5]
    sx = jnp.tanh(cam[0] * mx + cam[1] * my + cam[2] * mz + cam[3])
    sy = jnp.tanh(cam[4] * mx + cam[5] * my + cam[6] * mz + cam[7])
    spread = jnp.exp(-2.0 * ls)
    sop = sigmoid(op)
    amp = 0.3 * sop * live
    shade = sigmoid(picked[5:8])
    shade8 = jnp.concatenate([shade, jnp.zeros((5, slots), F32)], axis=0)
    steep = (-0.5 * LOG2E) * jnp.minimum(spread, 1e38)
    cols = jnp.concatenate([sx, sy, steep, amp, jnp.zeros((4, slots), F32)], axis=0).T
    cuts = [slice(b * K, (b + 1) * K) for b in range(tiles)]

    alphas, inverses, logs = [], [], []
    for cut in cuts:
        csx, csy, csp, camp = [cols[cut, n : n + 1] for n in range(4)]
        dx = across - csx
        dy = down - csy
        alpha = camp * jnp.exp2((dx * dx + dy * dy) * csp)
        rest = 1.0 - alpha
        alphas.append(alpha)
        inverses.append(alpha / rest)
        logs.append(jnp.concatenate(split(jnp.log(rest)), axis=0))
    befores = [mm(lower, x, NN) for x in logs]
    weights = [alpha * jnp.exp(before) for alpha, before in zip(alphas, befores)]
    packed = [weight.astype(BF16) for weight in weights]
    shade_hi, shade_lo = split(shade8)
    shade_two = jnp.concatenate([shade_hi, shade_lo], axis=0)
    colours = []
    for cut, weight in zip(cuts, packed):
        both = mm(shade_two[:, cut], weight, NN)
        colours.append(both[:8] + both[8:])
    loss_part = jnp.zeros((1, K), F32)
    dcols = []
    for b in range(tiles):
        want = jnp.concatenate(
            [want_ref[pl.ds(b, 1), c * pix : (c + 1) * pix].astype(F32) for c in range(3)]
            + [jnp.zeros((5, pix), F32)],
            axis=0,
        )
        for c in range(3):
            image_ref[pl.ds(b, 1), c * pix : (c + 1) * pix] = colours[b][c : c + 1].astype(BF16)
        diff = colours[b] - want
        sq = jnp.sum(diff * diff, axis=0, keepdims=True)
        for n in range(0, pix, K):
            loss_part = loss_part + sq[:, n : n + K]
        dcols.append(((2.0 * factor) * diff).astype(BF16))
    losses[me] = loss_part * factor
    dshade = jnp.concatenate([mm(d, w, NT) for d, w in zip(dcols, packed)], axis=1)
    dwws = [
        mm(shade_hi[:, cut], d, TN) * weight for cut, d, weight in zip(cuts, dcols, weights)
    ]
    dlogs = [mm(upper[:, :K], x.astype(BF16), NN) for x in dwws]
    sums = []
    for x, y, inverse in zip(dwws, dlogs, inverses):
        h = x - y * inverse
        both = mm(moments, jnp.concatenate(split(h), axis=0), NT)
        sums.append(both[:, :K] + both[:, K:])
    sums = jnp.concatenate(sums, axis=1)
    s_h, s_u, s_v, s_q = [sums[n : n + 1] for n in range(4)]
    s_x = s_u - sx * s_h
    s_y = s_v - sy * s_h
    s_r = s_q - 2.0 * (sx * s_u + sy * s_v) + (sx * sx + sy * sy) * s_h
    px = spread * s_x * (1.0 - sx * sx)
    py = spread * s_y * (1.0 - sy * sy)
    out = jnp.concatenate(
        [
            px,
            py,
            spread * s_r,
            (1.0 - sop) * s_h,
            dshade[0:3] * shade * (1.0 - shade),
            jnp.zeros((1, slots), F32),
        ],
        axis=0,
    )
    wide = slots // 2
    grads[me] = jnp.concatenate([out[:, :wide], out[:, wide:]], axis=0).astype(BF16)

    def push(n, buf, i, recv):
        j, to = peer(i)
        return pltpu.make_async_remote_copy(
            src_ref=buf.at[me], dst_ref=buf.at[me], send_sem=s_grad.at[n],
            recv_sem=recv, device_id=to, device_id_type=MESH,
        )

    @each_peer
    def _(i):
        push(0, grads, i, r_grad.at[me]).start()

    flow_all("x", 2).wait_recv()
    flow_all("y", 2).wait_recv()
    turn_line(1 - sec, lo)
    turn_line(sec, 1 - lo)

    def late_sends():
        flow_send("far_x", 2)
        flow_send("far_y", 2)

        @each_peer
        def _(i):
            push(1, losses, i, s_loss.at[1]).start()

    def gather_batch(g, n):
        sides = []
        for q in range(batch):
            i = source(g, q)
            j = peer(i)[0]
            if isinstance(i, int):
                if i > 0:
                    push(0, grads, i, r_grad.at[j]).wait_recv()
            else:
                pl.when(i > 0)(lambda: push(0, grads, i, r_grad.at[j]).wait_recv())
            got = grads[j]
            fit = fits[j]
            sides.append(
                jnp.concatenate(
                    [
                        jnp.concatenate(
                            [
                                fit[:, :wide] * got[p : p + 1],
                                fit[:, wide:] * got[PARAMS + p : PARAMS + p + 1],
                            ],
                            axis=1,
                        )
                        for p in range(ROWS)
                    ],
                    axis=0,
                )
            )
        return mm(jnp.concatenate(sides, axis=1), where[n], NT)

    def finish_turning():
        for name in ("far_x", "far_y"):
            for c in range(3):
                flow_all(name, c).wait_recv()
        turn_line(1 - sec, 1 - lo)

    last = group // batch - 1
    if ahead:
        for g in range(last + 1):
            if g == LATE:
                late_sends()
            if g == last + FINISH:
                finish_turning()
            if g < 2:
                dhead[g] = gather_batch(g, g)
            else:
                dhead[g % 2] += gather_batch(g, g)
        if FINISH > 0:
            finish_turning()
    else:
        late_sends()
        dhead[...] = jnp.zeros_like(dhead)

        @pl.loop(0, last + 1)
        def _(g):
            mark_rows(g, 0)
            dhead[g % 2] += gather_batch(g, 0)

        finish_turning()

    loss_all = losses.at[pl.ds(0, group - 1)]
    pltpu.make_async_remote_copy(
        src_ref=loss_all, dst_ref=loss_all, send_sem=s_grad.at[1], recv_sem=s_loss.at[1],
        device_id=partner, device_id_type=MESH,
    ).wait_recv()
    loss_mine[...] = jnp.broadcast_to(jnp.sum(losses[...], axis=0), loss_mine.shape)
    loss_copy = pltpu.make_async_remote_copy(
        src_ref=loss_mine, dst_ref=loss_theirs, send_sem=s_loss.at[0], recv_sem=r_loss,
        device_id=partner, device_id_type=MESH,
    )
    chunk = outw // 2
    dhead_rows = 256
    chunks = width // dhead_rows

    def part_copy(c):
        span = pl.ds(c * chunk, chunk)
        return pltpu.make_async_remote_copy(
            src_ref=mine.at[span], dst_ref=theirs.at[span],
            send_sem=s_part.at[c], recv_sem=r_part.at[c],
            device_id=partner, device_id_type=MESH,
        )

    def share(v, n):
        return dhead[v, n * gpt : (n + 1) * gpt]

    for p in [4, 5, 6, 7, 0, 1, 2, 3]:
        if p < 3:
            value = (
                cam[p] * share(0, 0) + cam[p + 4] * share(0, 1)
                + cam_far[p] * share(1, 0) + cam_far[p + 4] * share(1, 1)
            )
        else:
            value = share(0, p - 1) + share(1, p - 1)
        mine[p * gpt : (p + 1) * gpt] = value.astype(BF16)
        if (p + 1) * gpt % chunk == 0:
            part_copy((p + 1) * gpt // chunk - 1).start()
    loss_copy.start()

    def sides(buf, n):
        span = slice(n * dhead_rows, (n + 1) * dhead_rows)
        return span, jnp.concatenate([buf[m, span] for m in range(nsec * nlo)], axis=1)

    dh = mine[...]
    for n in range(chunks):
        span, side = sides(turned, n)
        grad_ref[span, :] = mm(side, dh, NT)
    turn_all = pltpu.make_async_remote_copy(
        src_ref=turned, dst_ref=turned_far, send_sem=s_turn, recv_sem=r_turn,
        device_id=partner, device_id_type=MESH,
    )
    turn_all.wait_recv()
    for c in (1, 0):
        part_copy(c).wait_recv()
        cut = slice(c * chunk, (c + 1) * chunk)
        dh = theirs[cut]
        for n in range(chunks):
            span, side = sides(turned_far, n)
            grad_ref[span, cut] += mm(side, dh, NT)
    loss_copy.wait_recv()
    loss_ref[...] = jnp.broadcast_to(
        jnp.sum(loss_mine[0:1] + loss_theirs[0:1], keepdims=True), loss_ref.shape
    )

    loss_copy.wait_send()
    for c in range(2):
        part_copy(c).wait_send()
    turn_all.wait_send()
    all_small(0, wanted).wait_send()
    all_small(1, lists).wait_send()
    all_small(2, given).wait_send()
    grad_all = grads.at[pl.ds(0, group - 1)]
    pltpu.make_async_remote_copy(
        src_ref=grad_all, dst_ref=grad_all, send_sem=s_grad.at[0], recv_sem=r_grad.at[0],
        device_id=partner, device_id_type=MESH,
    ).wait_send()
    pltpu.make_async_remote_copy(
        src_ref=loss_all, dst_ref=loss_all, send_sem=s_grad.at[1], recv_sem=s_loss.at[1],
        device_id=partner, device_id_type=MESH,
    ).wait_send()
    norm_copy(0, norms.at[pl.ds(0, group - 1)], partner).wait_send()


def store(image_ref, grad_ref, loss_ref, image_out, grad_out, loss_out, one, sems):
    rows = grad_ref.shape[0] // STORES
    pairs = [(image_ref, image_out), (one, loss_out)]
    for n in range(STORES):
        span = pl.ds(n * rows, rows)
        pairs.append((grad_ref.at[span], grad_out.at[span]))
    copies = [pltpu.make_async_copy(src, dst, sems.at[n]) for n, (src, dst) in enumerate(pairs)]
    one[...] = loss_ref[0:1, 0:1]
    for copy in copies:
        copy.start()
    for copy in copies:
        copy.wait()


def solution(mesh):
    nsec, nview, nscene = mesh.shape["section"], mesh.shape["view"], mesh.shape["scene"]
    group = nsec * nview
    nlo = 2
    assert nsec == 2 and nview % 8 == 0

    def body(tokens, norm_gain, head_weight, tile_lists, tile_counts, cameras, targets):
        tok_rows, width = tokens.shape[1:]
        outw = head_weight.shape[1]
        gpt = outw // PARAMS
        tiles, K = tile_lists.shape[1:]
        slots = tiles * K
        cap = 2 * slots // group
        packs = group * cap // 128
        factor = 1.0 / (nscene * tiles * group)
        ahead = group * group * tok_rows * slots <= 2**24
        batch = min(BATCH, group)
        vmem = pl.BlockSpec(memory_space=pltpu.VMEM)
        smem = pl.BlockSpec(memory_space=pltpu.SMEM)
        hbm = pl.BlockSpec(memory_space=pltpu.HBM)
        dma = pltpu.SemaphoreType.DMA
        image, grad, loss = pl.pallas_call(
            functools.partial(kernel, nsec, nview, factor),
            out_shape=(
                pltpu.VMEM((tiles, targets.shape[2]), BF16),
                pltpu.VMEM((width, outw), F32),
                pltpu.VMEM((8, 128), F32),
            ),
            in_specs=[hbm, hbm, hbm, hbm, smem, smem, hbm],
            out_specs=(vmem, vmem, vmem),
            scratch_shapes=[
                pltpu.VMEM((tok_rows, width), BF16),
                pltpu.VMEM((1, width), F32),
                pltpu.VMEM((width, outw), BF16),
                pltpu.VMEM((tiles, K), jnp.int32),
                pltpu.VMEM((tiles, targets.shape[2]), BF16),
                pltpu.VMEM((group * cap, slots), BF16),
                pltpu.VMEM((packs, 1, 128), F32),
                pltpu.VMEM((group, 1, 128), F32),
                pltpu.VMEM((packs, PARAMS, 128), BF16),
                pltpu.VMEM((group, PARAMS, 128), BF16),
                pltpu.VMEM((group, tiles, K), jnp.int32),
                pltpu.VMEM((group // batch if ahead else 1, group * tok_rows, batch * slots), BF16),
                pltpu.VMEM((group, gpt, slots), BF16),
                pltpu.VMEM((group, tok_rows, width), BF16),
                pltpu.VMEM((group, 2 * PARAMS, slots // 2), BF16),
                pltpu.VMEM((2, ROWS * gpt, group * tok_rows), F32),
                pltpu.VMEM((nsec * nlo, width, group * tok_rows // (nsec * nlo)), BF16),
                pltpu.VMEM((nsec * nlo, width, group * tok_rows // (nsec * nlo)), BF16),
                pltpu.VMEM((outw, group * tok_rows), BF16),
                pltpu.VMEM((outw, group * tok_rows), BF16),
                pltpu.VMEM((group, 1, K), F32),
                pltpu.VMEM((8, K), F32),
                pltpu.VMEM((8, K), F32),
                dma((5,)),
                dma((3,)), dma((3,)),
                dma, dma((15,)),
                dma((2,)), dma((group,)),
                dma((2,)), dma((2,)),
                dma((2,)), dma,
                dma, dma,
            ],
            compiler_params=pltpu.CompilerParams(
                collective_id=0, has_side_effects=True, vmem_limit_bytes=61 * 1024 * 1024
            ),
        )(
            tokens[0], norm_gain[None], head_weight, tile_lists[0], tile_counts[0], cameras[0],
            targets[0],
        )
        image, grad, loss = pl.pallas_call(
            store,
            out_shape=tuple(
                jax.ShapeDtypeStruct(shape, dtype)
                for shape, dtype in ((image.shape, BF16), (grad.shape, F32), ((1, 1), F32))
            ),
            in_specs=[vmem] * 3,
            out_specs=(hbm,) * 3,
            scratch_shapes=[pltpu.VMEM((1, 1), F32), dma((2 + STORES,))],
            compiler_params=pltpu.CompilerParams(vmem_limit_bytes=1024 * 1024),
        )(image, grad, loss)
        return image[None], grad, loss[0, 0]

    in_specs = (
        P("scene", ("section", "view"), None),
        P(),
        P(),
        P("scene", ("section", "view"), None),
        P("scene", ("section", "view")),
        P("scene", None, None),
        P("scene", ("section", "view"), None),
    )
    out_specs = (P("scene", ("section", "view"), None), P(), P())
    return jax.shard_map(body, mesh=mesh, in_specs=in_specs, out_specs=out_specs, check_vma=False)
```
